32 devices in a mesh: fsdp: 8 (over y, x, core), seq: 4 (over z).
Axes of the slice: x: 2, y: 2, z: 4, core: 2. Of those that a mesh axis runs over, the one named last changes fastest.
Arguments:
- tokens: bfloat16 [8, 2048, 4096], P('fsdp', 'seq'), may hold values from -72 to 72
- norm_gain: float32 [4096], replicated, may hold values from 0.1 to 1.9
- lru_proj: bfloat16 [4096, 2048], P(('fsdp', 'seq')), may hold values from -0.09375 to 0.09375
- gelu_proj: bfloat16 [4096, 2048], P(('fsdp', 'seq')), may hold values from -0.09375 to 0.09375
- conv_weight: float32 [4, 2048], replicated, may hold values from -3 to 3
- conv_bias: float32 [2048], replicated, may hold values from -3 to 3
- gate_weights: bfloat16 [2048, 512], P('seq'), may hold values from -0.375 to 0.375
- gate_bias: float32 [2, 2048], replicated, may hold values from -4 to 4
- decay_param: float32 [2048], replicated, may hold values from -13 to -2
Outputs:
- recurrent_out: bfloat16 [8, 2048, 2048], P('fsdp', 'seq')
The draws below stay inside these ranges and needn't reach their ends.
All inputs are finite; a program needn't handle non-finite values.
Results may differ from the reference program's by a relative error of at most 0.0051.
Values may be sent and summed in bfloat16 or wider, within the bound.
A program may use at most 128 MiB of HBM per device.

```python
import math
import jax
import jax.numpy as jnp
from jax import lax

D = 4096
BW = 256
H = 8
CONV = 4
TOK_DEV = 512
C = 2048
LENGTH = 2048
SEQS = 8


def draw_tokens(key, part):
    keys = jax.random.split(key, 3)
    shape = (SEQS, LENGTH, D)
    column_scale = jnp.exp(jax.random.uniform(keys[0], (D,), jnp.float32, math.log(0.3), math.log(3.0)))
    row_scale = jnp.exp(jax.random.uniform(keys[1], (SEQS, LENGTH, 1), jnp.float32, math.log(0.3), math.log(3.0)))
    base = jnp.clip(jax.random.normal(keys[2], shape, jnp.float32), -3.0, 3.0)
    return (base * row_scale * column_scale).astype(jnp.bfloat16)


def draw_decay_param(key, part):
    keys = jax.random.split(key, 3)
    shortest = min(40, TOK_DEV)
    slow_rate = jnp.exp(jax.random.uniform(keys[0], (C,), jnp.float32, math.log(0.05 / LENGTH), math.log(0.5 / LENGTH)))
    fast_rate = jnp.exp(jax.random.uniform(keys[1], (C,), jnp.float32, math.log(0.2 / shortest), math.log(0.5 / shortest)))
    share = 0.5
    picked = jax.random.uniform(keys[2], (C,), jnp.float32) < share
    rate = jnp.where(picked, fast_rate, slow_rate)
    return jnp.log(jnp.expm1(rate)).astype(jnp.float32)


def block_levels(key, dims, cuts, smallest, high):
    def one(position, blocks):
        draws = jax.random.uniform(jax.random.fold_in(jax.random.fold_in(key, 6), position), (blocks,), jnp.float32, smallest / len(cuts), high / len(cuts))
        return jnp.repeat(jnp.exp(draws), dims[position] // blocks).reshape((-1,) + (1,) * (len(dims) - position - 1))

    factor_of = one(*cuts[0])
    for cut in cuts[1:]:
        factor_of = factor_of * one(*cut)
    return factor_of


def noise(stream_key, extent, width, bound, cuts=(), kind=jnp.bfloat16):
    values = jax.random.normal(stream_key, extent, jnp.float32) * width
    if len(cuts) > 0:
        values = block_levels(stream_key, extent, cuts, -0.22, 0.18) * values
    return jnp.clip(values, min=-bound, max=bound).astype(kind)


def setup_inputs(seed: int = 0) -> dict:
    streams_of = jax.random.split(jax.random.key(seed), 10)
    return {
        "tokens": draw_tokens(jax.random.fold_in(streams_of[9], 71), 0),
        "norm_gain": jnp.clip(1.0 + 0.18 * jax.random.normal(streams_of[1], (D,), jnp.float32), 0.1, 1.9),
        "lru_proj": noise(streams_of[2], (D, C), D ** -0.5, 0.09375, ((0, 32),)),
        "gelu_proj": noise(streams_of[3], (D, C), D ** -0.5, 0.09375, ((0, 32),)),
        "conv_weight": noise(streams_of[4], (CONV, C), 0.5, 3.0, (), jnp.float32),
        "conv_bias": noise(streams_of[5], (C,), 0.5, 3.0, (), jnp.float32),
        "gate_weights": noise(streams_of[6], (C, 2 * BW), BW ** -0.5, 0.375, ((0, 4),)),
        "gate_bias": noise(streams_of[7], (2, C), 1.0, 4.0, (), jnp.float32),
        "decay_param": draw_decay_param(jax.random.fold_in(streams_of[9], 71), 0),
    }


def reference(tokens, norm_gain, lru_proj, gelu_proj, conv_weight, conv_bias, gate_weights, gate_bias, decay_param):

    def one_sequence(rows):
        values = rows.astype(jnp.float32)
        mean_square = lax.optimization_barrier(jnp.mean(values * values, axis=-1, keepdims=True))
        normed = (values * lax.rsqrt(mean_square + 1e-06) * norm_gain).astype(jnp.bfloat16)
        recurrent_in = jnp.dot(normed, lru_proj, preferred_element_type=jnp.float32).astype(jnp.bfloat16)
        gelu_in = jnp.dot(normed, gelu_proj, preferred_element_type=jnp.float32)
        padded = jnp.concatenate([jnp.zeros((CONV - 1, C), jnp.bfloat16), recurrent_in], axis=0)
        conv_sum = jnp.zeros((LENGTH, C), jnp.float32) + conv_bias
        for tap_index in range(CONV):
            begin = CONV - 1 - tap_index
            conv_sum = conv_sum + conv_weight[tap_index] * padded[begin:begin + LENGTH].astype(jnp.float32)
        conv_out = conv_sum.astype(jnp.bfloat16)
        gate_all = jnp.einsum('lhi,hij->lhj', conv_out.astype(jnp.float32).reshape(LENGTH, H, BW), gate_weights.astype(jnp.float32).reshape(H, BW, 2 * BW))
        input_gate = jax.nn.sigmoid(gate_all[:, :, :BW].reshape(LENGTH, C) + gate_bias[0])
        recur_gate = jax.nn.sigmoid(gate_all[:, :, BW:].reshape(LENGTH, C) + gate_bias[1])
        log_decay = -8.0 * jax.nn.softplus(decay_param) * recur_gate
        decay = jnp.exp(log_decay)
        driven = jnp.sqrt(-jnp.expm1(2.0 * log_decay)) * input_gate * conv_out.astype(jnp.float32)

        def advance(state, inputs):
            decay_now, driven_now = inputs
            state = decay_now * state + driven_now
            return (state, state)
        unused, states = lax.scan(advance, jnp.zeros((C,), jnp.float32), (decay, driven))
        return (states * jax.nn.gelu(gelu_in, approximate=True)).astype(jnp.bfloat16)
    return lax.map(one_sequence, tokens)
```

```python
import functools

import jax
import jax.numpy as jnp
from jax import lax
from jax.experimental import pallas as pl
from jax.experimental.pallas import tpu as pltpu
from jax.sharding import PartitionSpec as P

MESH = pl.DeviceIdType.MESH
LANES = 128
VMEM_BYTES = 66_000_000


def normalise(tokens_ref, gain_ref, normed_ref):
    rows = 32

    def body(i, _):
        at = pl.ds(pl.multiple_of(i * rows, rows), rows)
        values = tokens_ref[at, :].astype(jnp.float32)
        mean_square = jnp.mean(values * values, axis=-1, keepdims=True)
        normed_ref[at, :] = (values * lax.rsqrt(mean_square + 1e-06) * gain_ref[...]).astype(jnp.bfloat16)
        return 0

    lax.fori_loop(0, tokens_ref.shape[0] // rows, body, 0)


def gather_kernel(
    nz,
    tokens_ref, gain_ref, lru_ref, gelu_ref, gate_ref,
    rec_ref, act_ref, table_ref,
    w_ref, normed_ref, own_sem, send_sem, core_send, gate_send,
    z_recv, gate_recv, x_recv, y_recv, a_recv, b_recv, core_recv,
):
    f = lax.axis_index("fsdp")
    z = lax.axis_index("seq")
    c, x, y = f % 2, (f // 2) % 2, f // 4
    fx, fy, fc = f + 2 - 4 * x, f + 4 - 8 * y, f + 1 - 2 * c
    fd = fx + 4 - 8 * y
    shard = lru_ref.shape[0]
    line = shard * nz
    half = line // 2
    chunks = w_ref.shape[0]
    split = chunks // 2
    gate_rows = gate_ref.shape[0]
    piece = gate_rows // split

    def remote(src, send, recv, device):
        return pltpu.make_async_remote_copy(
            src_ref=src, dst_ref=src, send_sem=send, recv_sem=recv,
            device_id=device, device_id_type=MESH,
        )

    own = pl.ds(pl.multiple_of((f * nz + z) * shard, shard), shard)
    for t in range(chunks):
        src = lru_ref if t < split else gelu_ref
        cols = pl.ds((t % split) * LANES, LANES)
        pltpu.make_async_copy(src.at[:, cols], w_ref.at[t, own], own_sem.at[0]).start()
    own_gate = pl.ds(pl.multiple_of(z * gate_rows, gate_rows), gate_rows)
    gate_copy = pltpu.make_async_copy(gate_ref, table_ref.at[own_gate], own_sem.at[1])
    gate_copy.start()

    barrier = pltpu.get_barrier_semaphore()
    for device in ((fx, z), (fy, z), (fc, z)):
        pl.semaphore_signal(barrier, inc=1, device_id=device, device_id_type=MESH)

    @pl.when(z > 0)
    def _():
        pl.semaphore_signal(barrier, inc=1, device_id=(f, z - 1), device_id_type=MESH)

    @pl.when(z < nz - 1)
    def _():
        pl.semaphore_signal(barrier, inc=1, device_id=(f, z + 1), device_id_type=MESH)

    for k in range(nz):
        @pl.when(z == k)
        def _():
            pl.semaphore_wait(barrier, 3 + int(k > 0) + int(k < nz - 1))

    pltpu.make_async_copy(w_ref.at[:, own], w_ref.at[:, own], own_sem.at[0]).wait()
    gate_copy.wait()

    def shard_of(t, source):
        at = pl.ds(pl.multiple_of((f * nz + source) * shard, shard), shard)
        return w_ref.at[t, at]

    def gate_of(t, source):
        at = pl.ds(pl.multiple_of(source * gate_rows + t * piece, piece), piece)
        return table_ref.at[at]

    def pass_on(t, source, target):
        remote(shard_of(t, source), send_sem.at[t], z_recv.at[t, source], (f, target)).start()

        @pl.when(t < split)
        def _():
            remote(gate_of(t, source), gate_send.at[t], gate_recv.at[t, source], (f, target)).start()

    def arrived(t, source):
        remote(shard_of(t, source), send_sem.at[t], z_recv.at[t, source], (f, z)).wait_recv()

        @pl.when(t < split)
        def _():
            remote(gate_of(t, source), gate_send.at[t], gate_recv.at[t, source], (f, z)).wait_recv()

    def z_first(t):
        @pl.when(z > 0)
        def _():
            pass_on(t, z, z - 1)

        @pl.when(z < nz - 1)
        def _():
            pass_on(t, z, z + 1)

    def z_hop(t, distance):
        @pl.when(z >= distance)
        def _():
            arrived(t, z - distance)

            @pl.when(z < nz - 1)
            def _():
                pass_on(t, z - distance, z + 1)

        @pl.when(z + distance < nz)
        def _():
            arrived(t, z + distance)

            @pl.when(z > 0)
            def _():
                pass_on(t, z + distance, z - 1)

    def rows_of(owner, t, start, size):
        return w_ref.at[t, pl.ds(pl.multiple_of(owner * line + start, shard), size)]

    def to_core(t, owner, start, size):
        remote(rows_of(owner, t, start, size), core_send.at[t], core_recv.at[t], (fc, z)).start()

    def line_done(t):
        mine = rows_of(f, t, 0, line)
        remote(mine, send_sem.at[t], x_recv.at[t], (fx, z)).start()
        remote(mine, send_sem.at[t], y_recv.at[t], (fy, z)).start()
        to_core(t, f, 0, line)

    def sides_done(t):
        from_x = rows_of(fx, t, 0, line)
        remote(from_x, send_sem.at[t], x_recv.at[t], (fx, z)).wait_recv()
        remote(rows_of(fx, t, 0, half), send_sem.at[t], a_recv.at[t], (fy, z)).start()
        to_core(t, fx, 0, line)
        from_y = rows_of(fy, t, 0, line)
        remote(from_y, send_sem.at[t], y_recv.at[t], (fy, z)).wait_recv()
        remote(rows_of(fy, t, half, half), send_sem.at[t], b_recv.at[t], (fx, z)).start()
        to_core(t, fy, 0, line)

    def corner_done(t):
        remote(rows_of(fd, t, 0, half), send_sem.at[t], a_recv.at[t], (fy, z)).wait_recv()
        to_core(t, fd, 0, half)
        remote(rows_of(fd, t, half, half), send_sem.at[t], b_recv.at[t], (fx, z)).wait_recv()
        to_core(t, fd, half, half)

    def multiply(t):
        whole = w_ref.at[t, pl.ds(0, 4 * line)]
        pltpu.make_async_copy(whole, whole, core_recv.at[t]).wait()
        blocks = normed_ref.shape[0] // 256
        column = pl.ds(pl.multiple_of((t % split) * LANES, LANES), LANES)

        def body(i, _):
            at = pl.ds(pl.multiple_of(i * 256, 256), 256)
            product = jnp.dot(normed_ref[at, :], w_ref[t], preferred_element_type=jnp.float32)

            @pl.when(t < split)
            def _():
                rec_ref[at, column] = product.astype(jnp.bfloat16)

            @pl.when(t >= split)
            def _():
                act_ref[at, column] = product

            return 0

        lax.fori_loop(0, blocks, body, 0)

    stages = [z_first]
    for distance in range(1, nz):
        stages.append(functools.partial(z_hop, distance=distance))
    stages += [line_done, sides_done, corner_done, multiply]
    lags = list(range(nz)) + [nz - 1, nz, nz + 1, nz + 2]

    def step(t, _):
        for stage, lag in zip(stages, lags):
            @pl.when((t >= lag) & (t < chunks + lag))
            def _():
                stage(t - lag)

        @pl.when(t == 0)
        def _():
            normalise(tokens_ref, gain_ref, normed_ref)

        return 0

    lax.fori_loop(0, chunks + lags[-1], step, 0)

    def drain(t, _):
        for k in range(nz):
            shards_sent = (k + 1 if k < nz - 1 else 0) + (nz - k if k > 0 else 0)

            @pl.when(z == k)
            def _():
                sent = w_ref.at[t, pl.ds(0, shards_sent * shard + 3 * line)]
                pltpu.make_async_copy(sent, sent, send_sem.at[t]).wait()

                @pl.when(t < split)
                def _():
                    sent_gate = table_ref.at[pl.ds(0, shards_sent * piece)]
                    pltpu.make_async_copy(sent_gate, sent_gate, gate_send.at[t]).wait()

        whole = w_ref.at[t, pl.ds(0, 4 * line)]
        pltpu.make_async_copy(whole, whole, core_send.at[t]).wait()
        return 0

    lax.fori_loop(0, chunks, drain, 0)


def gathered_products(nz, tokens, norm_gain, lru_proj, gelu_proj, gate_weights):
    rows, width = tokens.shape
    inner = lru_proj.shape[1]
    chunks = 2 * inner // LANES
    vmem = pl.BlockSpec(memory_space=pltpu.VMEM)
    any_ = pl.BlockSpec(memory_space=pl.ANY)
    dma = pltpu.SemaphoreType.DMA
    return pl.pallas_call(
        functools.partial(gather_kernel, nz),
        out_shape=(
            jax.ShapeDtypeStruct((rows, inner), jnp.bfloat16),
            jax.ShapeDtypeStruct((rows, inner), jnp.float32),
            jax.ShapeDtypeStruct((gate_weights.shape[0] * nz, gate_weights.shape[1]), jnp.bfloat16),
        ),
        in_specs=[vmem, vmem, any_, any_, any_],
        out_specs=(vmem, vmem, vmem),
        scratch_shapes=[
            pltpu.VMEM((chunks, width, LANES), jnp.bfloat16),
            pltpu.VMEM((rows, width), jnp.bfloat16),
            dma((2,)), dma((chunks,)), dma((chunks,)), dma((chunks // 2,)),
            dma((chunks, nz)), dma((chunks // 2, nz)),
            dma((chunks,)), dma((chunks,)), dma((chunks,)), dma((chunks,)), dma((chunks,)),
        ],
        compiler_params=pltpu.CompilerParams(
            collective_id=0, has_side_effects=True, vmem_limit_bytes=VMEM_BYTES
        ),
    )(tokens, norm_gain.reshape(1, width), lru_proj, gelu_proj, gate_weights)


def scan_kernel(
    rec_ref, before_ref, weight_ref, bias_ref, table_ref, gate_bias_ref, decay_ref,
    state_ref, cumulative_ref, end_ref, padded_ref, a_ref, b_ref,
):
    rows, channels = rec_ref.shape
    taps = weight_ref.shape[0]
    lead = before_ref.shape[0]
    padded_ref[pl.ds(0, lead), :] = before_ref[...].astype(jnp.float32)
    padded_ref[pl.ds(lead, rows), :] = rec_ref[...].astype(jnp.float32)
    conv_sum = jnp.zeros((rows, channels), jnp.float32) + bias_ref[...]
    for tap in range(taps):
        conv_sum = conv_sum + weight_ref[tap : tap + 1, :] * padded_ref[pl.ds(lead - tap, rows), :]
    conv_out = conv_sum.astype(jnp.bfloat16)
    gates = jnp.dot(conv_out, table_ref[...], preferred_element_type=jnp.float32)
    input_gate = jax.nn.sigmoid(gates[:, :channels] + gate_bias_ref[0:1, :])
    recur_gate = jax.nn.sigmoid(gates[:, channels:] + gate_bias_ref[1:2, :])
    param = decay_ref[...]
    softplus = jnp.maximum(param, 0.0) + jnp.log1p(jnp.exp(-jnp.abs(param)))
    log_decay = -8.0 * softplus * recur_gate
    decay = jnp.exp(log_decay)
    lost = -jnp.tanh(log_decay) * (decay * decay + 1.0)
    driven = jnp.sqrt(lost) * input_gate * conv_out.astype(jnp.float32)
    parts = channels // LANES
    for j in range(parts):
        a_ref[j] = decay[:, j * LANES : (j + 1) * LANES]
        b_ref[j] = driven[:, j * LANES : (j + 1) * LANES]

    lanes = 8
    length = rows // lanes

    def body(i, carry):
        at = pl.ds(i, lanes, stride=length)
        after = []
        for j in range(parts):
            product, state = carry[j]
            decay_now = a_ref[j, at, :]
            product = product * decay_now
            state = decay_now * state + b_ref[j, at, :]
            a_ref[j, at, :] = product
            b_ref[j, at, :] = state
            after.append((product, state))
        return tuple(after)

    fresh = (jnp.ones((lanes, LANES), jnp.float32), jnp.zeros((lanes, LANES), jnp.float32))
    totals = lax.fori_loop(0, length, body, (fresh,) * parts, unroll=8)
    for j in range(parts):
        product, state = totals[j]
        cols = slice(j * LANES, (j + 1) * LANES)
        start = jnp.zeros((1, LANES), jnp.float32)
        prefix = jnp.ones((1, LANES), jnp.float32)
        for i in range(lanes):
            at = pl.ds(i * length, length)
            within = a_ref[j, at, :]
            state_ref[at, cols] = b_ref[j, at, :] + within * start
            cumulative_ref[at, cols] = within * prefix
            start = product[i : i + 1, :] * start + state[i : i + 1, :]
            prefix = prefix * product[i : i + 1, :]
        end_ref[0:1, cols] = prefix
        end_ref[1:2, cols] = start


def local_scan(rec, before, conv_weight, conv_bias, table, gate_bias, decay_param):
    rows, inner = rec.shape
    width = table.shape[1] // 2
    lead = before.shape[0]

    def columns(height):
        return pl.BlockSpec((height, width), lambda h: (0, h))

    return pl.pallas_call(
        scan_kernel,
        grid=(inner // width,),
        out_shape=(
            jax.ShapeDtypeStruct((rows, inner), jnp.float32),
            jax.ShapeDtypeStruct((rows, inner), jnp.float32),
            jax.ShapeDtypeStruct((2, inner), jnp.float32),
        ),
        in_specs=[
            columns(rows), columns(lead), columns(conv_weight.shape[0]), columns(1),
            pl.BlockSpec((width, 2 * width), lambda h: (h, 0)), columns(2), columns(1),
        ],
        out_specs=(columns(rows), columns(rows), columns(2)),
        scratch_shapes=[
            pltpu.VMEM((rows + lead, width), jnp.float32),
            pltpu.VMEM((width // LANES, rows, LANES), jnp.float32),
            pltpu.VMEM((width // LANES, rows, LANES), jnp.float32),
        ],
    )(
        rec, before, conv_weight, conv_bias.reshape(1, inner), table, gate_bias,
        decay_param.reshape(1, inner),
    )


def shards(
    nz, paired, tokens, norm_gain, lru_proj, gelu_proj, conv_weight, conv_bias, gate_weights,
    gate_bias, decay_param,
):
    seq_count, tok_rows, width = tokens.shape
    inner = lru_proj.shape[1]
    taps = conv_weight.shape[0]
    if paired:
        rec, act, table = gathered_products(
            nz, tokens.reshape(tok_rows, width), norm_gain, lru_proj, gelu_proj, gate_weights
        )
    else:
        flat = tokens.reshape(tok_rows, width).astype(jnp.float32)
        mean_square = jnp.mean(flat * flat, axis=-1, keepdims=True)
        normed = (flat * lax.rsqrt(mean_square + 1e-06) * norm_gain).astype(jnp.bfloat16)
        every = [
            lax.all_gather(w, ("fsdp", "seq"), axis=0, tiled=True) for w in (lru_proj, gelu_proj)
        ]
        rec = jnp.dot(normed, every[0], preferred_element_type=jnp.float32).astype(jnp.bfloat16)
        act = jnp.dot(normed, every[1], preferred_element_type=jnp.float32)
        table = lax.all_gather(gate_weights, "seq", axis=0, tiled=True)
    lead = 8
    before = lax.ppermute(
        rec[tok_rows - lead :, :], "seq", [(i, i + 1) for i in range(nz - 1)]
    )
    local, cumulative, ends = local_scan(
        rec, before, conv_weight, conv_bias, table, gate_bias, decay_param
    )
    every_end = lax.all_gather(ends, "seq")
    position = lax.axis_index("seq")
    start = jnp.zeros((inner,), jnp.float32)
    for k in range(nz - 1):
        start = jnp.where(k < position, every_end[k, 0] * start + every_end[k, 1], start)
    gelu = jax.nn.gelu(act, approximate=True)
    out = ((local + cumulative * start) * gelu).astype(jnp.bfloat16)
    return out.reshape(seq_count, tok_rows, inner)


def solution(mesh):
    placed = (
        P("fsdp", "seq", None), P(), P(("fsdp", "seq"), None), P(("fsdp", "seq"), None), P(), P(),
        P("seq", None), P(), P(),
    )
    nz = mesh.shape["seq"]
    paired = mesh.shape["fsdp"] == 8
    return jax.shard_map(
        functools.partial(shards, nz, paired), mesh=mesh, in_specs=placed,
        out_specs=P("fsdp", "seq", None), check_vma=False,
    )
```

```python
import functools

import jax
import jax.numpy as jnp
from jax import lax
from jax.experimental import pallas as pl
from jax.experimental.pallas import tpu as pltpu
from jax.sharding import PartitionSpec as P

MESH = pl.DeviceIdType.MESH
LANES = 128
VMEM_BYTES = 66_000_000


def normalise(tokens_ref, gain_ref, normed_ref):
    rows = 32

    def body(i, _):
        at = pl.ds(pl.multiple_of(i * rows, rows), rows)
        values = tokens_ref[at, :].astype(jnp.float32)
        mean_square = jnp.mean(values * values, axis=-1, keepdims=True)
        normed_ref[at, :] = (values * lax.rsqrt(mean_square + 1e-06) * gain_ref[...]).astype(jnp.bfloat16)
        return 0

    lax.fori_loop(0, tokens_ref.shape[0] // rows, body, 0)


def branch_kernel(
    nz,
    tokens_ref, gain_ref, lru_ref, gelu_ref, gate_ref,
    weight_ref, bias_ref, gate_bias_ref, decay_ref,
    out_ref,
    w_ref, normed_ref, rec_ref, table_ref, before_ref, padded_ref, a_ref, b_ref,
    end_ref, carry_ref, start_ref,
    own_sem, send_sem, core_send, gate_send, gate_core_send, tail_send, carry_send,
    z_recv, gate_recv, gate_core_recv, x_recv, y_recv, a_recv, b_recv, core_recv,
    tail_recv, carry_recv,
):
    f = lax.axis_index("fsdp")
    z = lax.axis_index("seq")
    c, x, y = f % 2, (f // 2) % 2, f // 4
    fx, fy, fc = f + 2 - 4 * x, f + 4 - 8 * y, f + 1 - 2 * c
    fd = fx + 4 - 8 * y
    shard = lru_ref.shape[0]
    line = shard * nz
    half = line // 2
    chunks = w_ref.shape[0]
    split = chunks // 2
    gate_rows = gate_ref.shape[0]
    gate_steps = split // 2
    piece = gate_rows // 2 // gate_steps
    rows = normed_ref.shape[0]
    channels = table_ref.shape[1] // 2
    heads = rec_ref.shape[1] // channels
    pieces = channels // LANES
    taps = weight_ref.shape[0]
    lead = before_ref.shape[0]

    def remote(src, send, recv, device):
        return pltpu.make_async_remote_copy(
            src_ref=src, dst_ref=src, send_sem=send, recv_sem=recv,
            device_id=device, device_id_type=MESH,
        )

    own = pl.ds(pl.multiple_of((f * nz + z) * shard, shard), shard)
    for t in range(chunks):
        src = lru_ref if t < split else gelu_ref
        cols = pl.ds((t % split) * LANES, LANES)
        pltpu.make_async_copy(src.at[:, cols], w_ref.at[t, own], own_sem.at[0]).start()
    own_gate = pl.ds(pl.multiple_of(z * gate_rows, gate_rows), gate_rows)
    gate_copy = pltpu.make_async_copy(gate_ref, table_ref.at[own_gate], own_sem.at[1])
    gate_copy.start()

    barrier = pltpu.get_barrier_semaphore()
    for device in ((fx, z), (fy, z), (fc, z)):
        pl.semaphore_signal(barrier, inc=1, device_id=device, device_id_type=MESH)

    @pl.when(z > 0)
    def _():
        pl.semaphore_signal(barrier, inc=1, device_id=(f, z - 1), device_id_type=MESH)

    @pl.when(z < nz - 1)
    def _():
        pl.semaphore_signal(barrier, inc=1, device_id=(f, z + 1), device_id_type=MESH)

    for k in range(nz):
        @pl.when(z == k)
        def _():
            pl.semaphore_wait(barrier, 3 + int(k > 0) + int(k < nz - 1))

    pltpu.make_async_copy(w_ref.at[:, own], w_ref.at[:, own], own_sem.at[0]).wait()
    gate_copy.wait()

    def shard_of(t, source):
        at = pl.ds(pl.multiple_of((f * nz + source) * shard, shard), shard)
        return w_ref.at[t, at]

    def gate_of(t, source):
        first = source * gate_rows + c * (gate_rows // 2) + t * piece
        return table_ref.at[pl.ds(pl.multiple_of(first, piece), piece)]

    def pass_on(t, source, target):
        remote(shard_of(t, source), send_sem.at[t], z_recv.at[t, source], (f, target)).start()

        @pl.when(t < gate_steps)
        def _():
            remote(gate_of(t, source), gate_send.at[t], gate_recv.at[t, source], (f, target)).start()

    def arrived(t, source):
        remote(shard_of(t, source), send_sem.at[t], z_recv.at[t, source], (f, z)).wait_recv()

        @pl.when(t < gate_steps)
        def _():
            remote(gate_of(t, source), gate_send.at[t], gate_recv.at[t, source], (f, z)).wait_recv()

    def z_first(t):
        @pl.when(z > 0)
        def _():
            pass_on(t, z, z - 1)

        @pl.when(z < nz - 1)
        def _():
            pass_on(t, z, z + 1)

    def z_hop(t, distance):
        @pl.when(z >= distance)
        def _():
            arrived(t, z - distance)

            @pl.when(z < nz - 1)
            def _():
                pass_on(t, z - distance, z + 1)

        @pl.when(z + distance < nz)
        def _():
            arrived(t, z + distance)

            @pl.when(z > 0)
            def _():
                pass_on(t, z + distance, z - 1)

    def rows_of(owner, t, start, size):
        return w_ref.at[t, pl.ds(pl.multiple_of(owner * line + start, shard), size)]

    def to_core(t, owner, start, size):
        remote(rows_of(owner, t, start, size), core_send.at[t], core_recv.at[t], (fc, z)).start()

    def line_done(t):
        mine = rows_of(f, t, 0, line)
        remote(mine, send_sem.at[t], x_recv.at[t], (fx, z)).start()
        remote(mine, send_sem.at[t], y_recv.at[t], (fy, z)).start()
        to_core(t, f, 0, line)

        @pl.when(t < gate_steps)
        def _():
            for source in range(nz):
                @pl.when(z != source)
                def _():
                    remote(
                        gate_of(t, source), gate_core_send.at[t], gate_core_recv.at[t], (fc, z)
                    ).start()

    def gate_done(t):
        @pl.when(t < gate_steps)
        def _():
            others = table_ref.at[pl.ds(0, (nz - 1) * piece)]
            pltpu.make_async_copy(others, others, gate_core_recv.at[t]).wait()

    def sides_done(t):
        from_x = rows_of(fx, t, 0, line)
        remote(from_x, send_sem.at[t], x_recv.at[t], (fx, z)).wait_recv()
        remote(rows_of(fx, t, 0, half), send_sem.at[t], a_recv.at[t], (fy, z)).start()
        to_core(t, fx, 0, line)
        from_y = rows_of(fy, t, 0, line)
        remote(from_y, send_sem.at[t], y_recv.at[t], (fy, z)).wait_recv()
        remote(rows_of(fy, t, half, half), send_sem.at[t], b_recv.at[t], (fx, z)).start()
        to_core(t, fy, 0, line)

    def corner_done(t):
        remote(rows_of(fd, t, 0, half), send_sem.at[t], a_recv.at[t], (fy, z)).wait_recv()
        to_core(t, fd, 0, half)
        remote(rows_of(fd, t, half, half), send_sem.at[t], b_recv.at[t], (fx, z)).wait_recv()
        to_core(t, fd, half, half)

    def multiply(t):
        whole = w_ref.at[t, pl.ds(0, 4 * line)]
        pltpu.make_async_copy(whole, whole, core_recv.at[t]).wait()
        blocks = normed_ref.shape[0] // 256
        column = pl.ds(pl.multiple_of((t % split) * LANES, LANES), LANES)

        def body(i, _):
            at = pl.ds(pl.multiple_of(i * 256, 256), 256)
            product = jnp.dot(normed_ref[at, :], w_ref[t], preferred_element_type=jnp.float32)

            @pl.when(t < split)
            def _():
                rec_ref[at, column] = product.astype(jnp.bfloat16)

            @pl.when(t >= split)
            def _():
                chunk = jnp.maximum(t - split, 0)
                state = b_ref[chunk, at, :] + a_ref[chunk, at, :] * start_ref[0:1, column]
                out_ref[at, column] = (state * jax.nn.gelu(product, approximate=True)).astype(out_ref.dtype)

            return 0

        lax.fori_loop(0, blocks, body, 0)

    def columns(h):
        return pl.ds(pl.multiple_of(h * channels, channels), channels)

    def tail_copy(h, source_rows, device):
        return pltpu.make_async_remote_copy(
            src_ref=rec_ref.at[pl.ds(source_rows, lead), columns(h)],
            dst_ref=before_ref.at[:, columns(h)],
            send_sem=tail_send.at[h], recv_sem=tail_recv.at[h],
            device_id=device, device_id_type=MESH,
        )

    def carry_copy(h, device):
        return pltpu.make_async_remote_copy(
            src_ref=carry_ref.at[:, columns(h)], dst_ref=start_ref.at[:, columns(h)],
            send_sem=carry_send.at[h], recv_sem=carry_recv.at[h],
            device_id=device, device_id_type=MESH,
        )

    def send_tail(h):
        @pl.when(z < nz - 1)
        def _():
            tail_copy(h, rows - lead, (f, z + 1)).start()

    def scan(h):
        @pl.when(z > 0)
        def _():
            tail_copy(h, rows - lead, (f, z)).wait_recv()

        cols = columns(h)
        padded_ref[pl.ds(0, lead), :] = before_ref[:, cols].astype(jnp.float32)
        padded_ref[pl.ds(lead, rows), :] = rec_ref[:, cols].astype(jnp.float32)
        conv_sum = jnp.zeros((rows, channels), jnp.float32) + bias_ref[:, cols]
        for tap in range(taps):
            conv_sum = conv_sum + weight_ref[tap : tap + 1, cols] * padded_ref[pl.ds(lead - tap, rows), :]
        conv_out = conv_sum.astype(jnp.bfloat16)
        gates = jnp.dot(conv_out, table_ref[cols, :], preferred_element_type=jnp.float32)
        input_gate = jax.nn.sigmoid(gates[:, :channels] + gate_bias_ref[0:1, cols])
        recur_gate = jax.nn.sigmoid(gates[:, channels:] + gate_bias_ref[1:2, cols])
        param = decay_ref[:, cols]
        softplus = jnp.maximum(param, 0.0) + jnp.log1p(jnp.exp(-jnp.abs(param)))
        log_decay = -8.0 * softplus * recur_gate
        decay = jnp.exp(log_decay)
        lost = -jnp.tanh(log_decay) * (decay * decay + 1.0)
        driven = jnp.sqrt(lost) * input_gate * conv_out.astype(jnp.float32)
        for j in range(pieces):
            a_ref[h * pieces + j] = decay[:, j * LANES : (j + 1) * LANES]
            b_ref[h * pieces + j] = driven[:, j * LANES : (j + 1) * LANES]

        lanes = 8
        length = rows // lanes

        def body(i, carry):
            at = pl.ds(i, lanes, stride=length)
            after = []
            for j in range(pieces):
                product, state = carry[j]
                decay_now = a_ref[h * pieces + j, at, :]
                product = product * decay_now
                state = decay_now * state + b_ref[h * pieces + j, at, :]
                a_ref[h * pieces + j, at, :] = product
                b_ref[h * pieces + j, at, :] = state
                after.append((product, state))
            return tuple(after)

        fresh = (jnp.ones((lanes, LANES), jnp.float32), jnp.zeros((lanes, LANES), jnp.float32))
        totals = lax.fori_loop(0, length, body, (fresh,) * pieces, unroll=8)
        for j in range(pieces):
            product, state = totals[j]
            start = jnp.zeros((1, LANES), jnp.float32)
            prefix = jnp.ones((1, LANES), jnp.float32)
            for i in range(lanes):
                at = pl.ds(i * length, length)
                within = a_ref[h * pieces + j, at, :]
                b_ref[h * pieces + j, at, :] = b_ref[h * pieces + j, at, :] + within * start
                a_ref[h * pieces + j, at, :] = within * prefix
                start = product[i : i + 1, :] * start + state[i : i + 1, :]
                prefix = prefix * product[i : i + 1, :]
            col = pl.ds(pl.multiple_of((h * pieces + j) * LANES, LANES), LANES)
            end_ref[0:1, col] = prefix
            end_ref[1:2, col] = start

    def make_carry(h):
        cols = columns(h)

        @pl.when(z > 0)
        def _():
            carry_copy(h, (f, z)).wait_recv()

        @pl.when(z < nz - 1)
        def _():
            end = end_ref[0:1, cols] * start_ref[0:1, cols] + end_ref[1:2, cols]
            carry_ref[:, cols] = jnp.broadcast_to(end, (carry_ref.shape[0], channels))

    def send_carry(h):
        @pl.when(z < nz - 1)
        def _():
            carry_copy(h, (f, z + 1)).start()

    @pl.when(z == 0)
    def _():
        before_ref[...] = jnp.zeros_like(before_ref)
        start_ref[...] = jnp.zeros_like(start_ref)

    stages = [z_first]
    for distance in range(1, nz):
        stages.append(functools.partial(z_hop, distance=distance))
    stages += [line_done, sides_done, corner_done, gate_done, multiply]
    lags = list(range(nz)) + [nz - 1, nz, nz + 1, nz + 1, nz + 2]
    scan_at = gate_steps + nz

    def on_head(s, first, stage):
        @pl.when((s >= first) & (s < first + pieces * heads) & ((s - first) % pieces == 0))
        def _():
            stage((s - first) // pieces)

    def step(s, _):
        for stage, lag in zip(stages[:-1], lags[:-1]):
            @pl.when((s >= lag) & (s < chunks + lag))
            def _():
                stage(s - lag)

        on_head(s, scan_at + 2 + 2 * z, send_carry)
        on_head(s, nz + 2 + pieces, send_tail)

        @pl.when(s == 0)
        def _():
            normalise(tokens_ref, gain_ref, normed_ref)

        on_head(s, scan_at + 1 + 2 * z, make_carry)

        @pl.when((s >= lags[-1]) & (s < chunks + lags[-1]))
        def _():
            multiply(s - lags[-1])

        on_head(s, scan_at, scan)
        return 0

    lax.fori_loop(0, chunks + lags[-1], step, 0)

    def drain(t, _):
        for k in range(nz):
            shards_sent = (k + 1 if k < nz - 1 else 0) + (nz - k if k > 0 else 0)

            @pl.when(z == k)
            def _():
                sent = w_ref.at[t, pl.ds(0, shards_sent * shard + 3 * line)]
                pltpu.make_async_copy(sent, sent, send_sem.at[t]).wait()

                @pl.when(t < gate_steps)
                def _():
                    sent_gate = table_ref.at[pl.ds(0, shards_sent * piece)]
                    pltpu.make_async_copy(sent_gate, sent_gate, gate_send.at[t]).wait()

        whole = w_ref.at[t, pl.ds(0, 4 * line)]
        pltpu.make_async_copy(whole, whole, core_send.at[t]).wait()

        @pl.when(t < gate_steps)
        def _():
            others = table_ref.at[pl.ds(0, (nz - 1) * piece)]
            pltpu.make_async_copy(others, others, gate_core_send.at[t]).wait()

        @pl.when((t < heads) & (z < nz - 1))
        def _():
            tail_copy(t, rows - lead, (f, z)).wait_send()
            carry_copy(t, (f, z)).wait_send()

        return 0

    lax.fori_loop(0, chunks, drain, 0)


def fused_branch(
    nz, tokens, norm_gain, lru_proj, gelu_proj, conv_weight, conv_bias, gate_weights, gate_bias,
    decay_param,
):
    rows, width = tokens.shape
    inner = lru_proj.shape[1]
    chunks = 2 * inner // LANES
    channels = gate_weights.shape[1] // 2
    heads = inner // channels
    vmem = pl.BlockSpec(memory_space=pltpu.VMEM)
    any_ = pl.BlockSpec(memory_space=pl.ANY)
    dma = pltpu.SemaphoreType.DMA
    f32, bf16 = jnp.float32, jnp.bfloat16
    lead = 16
    return pl.pallas_call(
        functools.partial(branch_kernel, nz),
        out_shape=jax.ShapeDtypeStruct((rows, inner), bf16),
        in_specs=[vmem, vmem, any_, any_, any_, vmem, vmem, vmem, vmem],
        out_specs=vmem,
        scratch_shapes=[
            pltpu.VMEM((chunks, width, LANES), bf16),
            pltpu.VMEM((rows, width), bf16),
            pltpu.VMEM((rows, inner), bf16),
            pltpu.VMEM((gate_weights.shape[0] * nz, 2 * channels), bf16),
            pltpu.VMEM((lead, inner), bf16),
            pltpu.VMEM((lead + rows, channels), f32),
            pltpu.VMEM((chunks // 2, rows, LANES), f32),
            pltpu.VMEM((chunks // 2, rows, LANES), f32),
            pltpu.VMEM((8, inner), f32), pltpu.VMEM((8, inner), f32), pltpu.VMEM((8, inner), f32),
            dma((2,)), dma((chunks,)), dma((chunks,)), dma((chunks // 4,)), dma((chunks // 4,)),
            dma((heads,)), dma((heads,)),
            dma((chunks, nz)), dma((chunks // 4, nz)), dma((chunks // 4,)),
            dma((chunks,)), dma((chunks,)), dma((chunks,)), dma((chunks,)), dma((chunks,)),
            dma((heads,)), dma((heads,)),
        ],
        compiler_params=pltpu.CompilerParams(
            collective_id=0, has_side_effects=True, vmem_limit_bytes=VMEM_BYTES
        ),
    )(
        tokens, norm_gain.reshape(1, width), lru_proj, gelu_proj, gate_weights, conv_weight,
        conv_bias.reshape(1, inner), gate_bias, decay_param.reshape(1, inner),
    )


def scan_kernel(
    rec_ref, before_ref, weight_ref, bias_ref, table_ref, gate_bias_ref, decay_ref,
    state_ref, cumulative_ref, end_ref, padded_ref, a_ref, b_ref,
):
    rows, channels = rec_ref.shape
    taps = weight_ref.shape[0]
    lead = before_ref.shape[0]
    padded_ref[pl.ds(0, lead), :] = before_ref[...].astype(jnp.float32)
    padded_ref[pl.ds(lead, rows), :] = rec_ref[...].astype(jnp.float32)
    conv_sum = jnp.zeros((rows, channels), jnp.float32) + bias_ref[...]
    for tap in range(taps):
        conv_sum = conv_sum + weight_ref[tap : tap + 1, :] * padded_ref[pl.ds(lead - tap, rows), :]
    conv_out = conv_sum.astype(jnp.bfloat16)
    gates = jnp.dot(conv_out, table_ref[...], preferred_element_type=jnp.float32)
    input_gate = jax.nn.sigmoid(gates[:, :channels] + gate_bias_ref[0:1, :])
    recur_gate = jax.nn.sigmoid(gates[:, channels:] + gate_bias_ref[1:2, :])
    param = decay_ref[...]
    softplus = jnp.maximum(param, 0.0) + jnp.log1p(jnp.exp(-jnp.abs(param)))
    log_decay = -8.0 * softplus * recur_gate
    decay = jnp.exp(log_decay)
    lost = -jnp.tanh(log_decay) * (decay * decay + 1.0)
    driven = jnp.sqrt(lost) * input_gate * conv_out.astype(jnp.float32)
    parts = channels // LANES
    for j in range(parts):
        a_ref[j] = decay[:, j * LANES : (j + 1) * LANES]
        b_ref[j] = driven[:, j * LANES : (j + 1) * LANES]

    lanes = 8
    length = rows // lanes

    def body(i, carry):
        at = pl.ds(i, lanes, stride=length)
        after = []
        for j in range(parts):
            product, state = carry[j]
            decay_now = a_ref[j, at, :]
            product = product * decay_now
            state = decay_now * state + b_ref[j, at, :]
            a_ref[j, at, :] = product
            b_ref[j, at, :] = state
            after.append((product, state))
        return tuple(after)

    fresh = (jnp.ones((lanes, LANES), jnp.float32), jnp.zeros((lanes, LANES), jnp.float32))
    totals = lax.fori_loop(0, length, body, (fresh,) * parts, unroll=8)
    for j in range(parts):
        product, state = totals[j]
        cols = slice(j * LANES, (j + 1) * LANES)
        start = jnp.zeros((1, LANES), jnp.float32)
        prefix = jnp.ones((1, LANES), jnp.float32)
        for i in range(lanes):
            at = pl.ds(i * length, length)
            within = a_ref[j, at, :]
            state_ref[at, cols] = b_ref[j, at, :] + within * start
            cumulative_ref[at, cols] = within * prefix
            start = product[i : i + 1, :] * start + state[i : i + 1, :]
            prefix = prefix * product[i : i + 1, :]
        end_ref[0:1, cols] = prefix
        end_ref[1:2, cols] = start


def local_scan(rec, before, conv_weight, conv_bias, table, gate_bias, decay_param):
    rows, inner = rec.shape
    width = table.shape[1] // 2
    lead = before.shape[0]

    def columns(height):
        return pl.BlockSpec((height, width), lambda h: (0, h))

    return pl.pallas_call(
        scan_kernel,
        grid=(inner // width,),
        out_shape=(
            jax.ShapeDtypeStruct((rows, inner), jnp.float32),
            jax.ShapeDtypeStruct((rows, inner), jnp.float32),
            jax.ShapeDtypeStruct((2, inner), jnp.float32),
        ),
        in_specs=[
            columns(rows), columns(lead), columns(conv_weight.shape[0]), columns(1),
            pl.BlockSpec((width, 2 * width), lambda h: (h, 0)), columns(2), columns(1),
        ],
        out_specs=(columns(rows), columns(rows), columns(2)),
        scratch_shapes=[
            pltpu.VMEM((rows + lead, width), jnp.float32),
            pltpu.VMEM((width // LANES, rows, LANES), jnp.float32),
            pltpu.VMEM((width // LANES, rows, LANES), jnp.float32),
        ],
    )(
        rec, before, conv_weight, conv_bias.reshape(1, inner), table, gate_bias,
        decay_param.reshape(1, inner),
    )


def shards(
    nz, paired, tokens, norm_gain, lru_proj, gelu_proj, conv_weight, conv_bias, gate_weights,
    gate_bias, decay_param,
):
    seq_count, tok_rows, width = tokens.shape
    inner = lru_proj.shape[1]
    taps = conv_weight.shape[0]
    if paired:
        out = fused_branch(
            nz, tokens.reshape(tok_rows, width), norm_gain, lru_proj, gelu_proj, conv_weight,
            conv_bias, gate_weights, gate_bias, decay_param,
        )
        return out.reshape(seq_count, tok_rows, inner)
    flat = tokens.reshape(tok_rows, width).astype(jnp.float32)
    mean_square = jnp.mean(flat * flat, axis=-1, keepdims=True)
    normed = (flat * lax.rsqrt(mean_square + 1e-06) * norm_gain).astype(jnp.bfloat16)
    every = [
        lax.all_gather(w, ("fsdp", "seq"), axis=0, tiled=True) for w in (lru_proj, gelu_proj)
    ]
    rec = jnp.dot(normed, every[0], preferred_element_type=jnp.float32).astype(jnp.bfloat16)
    act = jnp.dot(normed, every[1], preferred_element_type=jnp.float32)
    table = lax.all_gather(gate_weights, "seq", axis=0, tiled=True)
    lead = 8
    before = lax.ppermute(
        rec[tok_rows - lead :, :], "seq", [(i, i + 1) for i in range(nz - 1)]
    )
    local, cumulative, ends = local_scan(
        rec, before, conv_weight, conv_bias, table, gate_bias, decay_param
    )
    every_end = lax.all_gather(ends, "seq")
    position = lax.axis_index("seq")
    start = jnp.zeros((inner,), jnp.float32)
    for k in range(nz - 1):
        start = jnp.where(k < position, every_end[k, 0] * start + every_end[k, 1], start)
    gelu = jax.nn.gelu(act, approximate=True)
    out = ((local + cumulative * start) * gelu).astype(jnp.bfloat16)
    return out.reshape(seq_count, tok_rows, inner)


def solution(mesh):
    placed = (
        P("fsdp", "seq", None), P(), P(("fsdp", "seq"), None), P(("fsdp", "seq"), None), P(), P(),
        P("seq", None), P(), P(),
    )
    nz = mesh.shape["seq"]
    paired = mesh.shape["fsdp"] == 8 and 1 < nz <= 5
    return jax.shard_map(
        functools.partial(shards, nz, paired), mesh=mesh, in_specs=placed,
        out_specs=P("fsdp", "seq", None), check_vma=False,
    )
```

```python
import functools

import jax
import jax.numpy as jnp
from jax import lax
from jax.experimental import pallas as pl
from jax.experimental.pallas import tpu as pltpu
from jax.sharding import PartitionSpec as P

MESH = pl.DeviceIdType.MESH
LANES = 128
VMEM_BYTES = 66_000_000


def normalise(tokens_ref, gain_ref, normed_ref):
    rows = 32

    def body(i, _):
        at = pl.ds(pl.multiple_of(i * rows, rows), rows)
        values = tokens_ref[at, :].astype(jnp.float32)
        mean_square = jnp.mean(values * values, axis=-1, keepdims=True)
        normed_ref[at, :] = (values * lax.rsqrt(mean_square + 1e-06) * gain_ref[...]).astype(jnp.bfloat16)
        return 0

    lax.fori_loop(0, tokens_ref.shape[0] // rows, body, 0)


def branch_kernel(
    nz,
    tokens_ref, gain_ref, lru_ref, gelu_ref, gate_ref,
    weight_ref, bias_ref, gate_bias_ref, decay_ref,
    out_ref,
    w_ref, normed_ref, rec_ref, table_ref, before_ref, padded_ref, a_ref, b_ref,
    end_ref, carry_ref, start_ref,
    own_sem, send_sem, core_send, gate_send, gate_core_send, tail_send, carry_send,
    z_recv, gate_recv, gate_core_recv, x_recv, y_recv, a_recv, b_recv, core_recv,
    tail_recv, carry_recv,
):
    f = lax.axis_index("fsdp")
    z = lax.axis_index("seq")
    c, x, y = f % 2, (f // 2) % 2, f // 4
    fx, fy, fc = f + 2 - 4 * x, f + 4 - 8 * y, f + 1 - 2 * c
    fd = fx + 4 - 8 * y
    shard = lru_ref.shape[0]
    line = shard * nz
    half = line // 2
    chunks = w_ref.shape[0]
    split = chunks // 2
    gate_rows = gate_ref.shape[0]
    gate_steps = split // 2
    piece = gate_rows // 2 // gate_steps
    rows = normed_ref.shape[0]
    channels = table_ref.shape[1] // 2
    heads = rec_ref.shape[1] // channels
    pieces = channels // LANES
    taps = weight_ref.shape[0]
    lead = before_ref.shape[0]

    def remote(src, send, recv, device):
        return pltpu.make_async_remote_copy(
            src_ref=src, dst_ref=src, send_sem=send, recv_sem=recv,
            device_id=device, device_id_type=MESH,
        )

    own = pl.ds(pl.multiple_of((f * nz + z) * shard, shard), shard)
    for t in range(chunks):
        src = lru_ref if t < split else gelu_ref
        cols = pl.ds((t % split) * LANES, LANES)
        pltpu.make_async_copy(src.at[:, cols], w_ref.at[t, own], own_sem.at[0]).start()
    own_gate = pl.ds(pl.multiple_of(z * gate_rows, gate_rows), gate_rows)
    gate_copy = pltpu.make_async_copy(gate_ref, table_ref.at[own_gate], own_sem.at[1])
    gate_copy.start()

    barrier = pltpu.get_barrier_semaphore()
    for device in ((fx, z), (fy, z), (fc, z)):
        pl.semaphore_signal(barrier, inc=1, device_id=device, device_id_type=MESH)

    @pl.when(z > 0)
    def _():
        pl.semaphore_signal(barrier, inc=1, device_id=(f, z - 1), device_id_type=MESH)

    @pl.when(z < nz - 1)
    def _():
        pl.semaphore_signal(barrier, inc=1, device_id=(f, z + 1), device_id_type=MESH)

    for k in range(nz):
        @pl.when(z == k)
        def _():
            pl.semaphore_wait(barrier, 3 + int(k > 0) + int(k < nz - 1))

    pltpu.make_async_copy(w_ref.at[:, own], w_ref.at[:, own], own_sem.at[0]).wait()
    gate_copy.wait()

    def shard_of(t, source):
        at = pl.ds(pl.multiple_of((f * nz + source) * shard, shard), shard)
        return w_ref.at[t, at]

    def gate_of(t, source):
        first = source * gate_rows + c * (gate_rows // 2) + t * piece
        return table_ref.at[pl.ds(pl.multiple_of(first, piece), piece)]

    def pass_on(t, source, target):
        remote(shard_of(t, source), send_sem.at[t], z_recv.at[t, source], (f, target)).start()

        @pl.when(t < gate_steps)
        def _():
            remote(gate_of(t, source), gate_send.at[t], gate_recv.at[t, source], (f, target)).start()

    def arrived(t, source):
        remote(shard_of(t, source), send_sem.at[t], z_recv.at[t, source], (f, z)).wait_recv()

        @pl.when(t < gate_steps)
        def _():
            remote(gate_of(t, source), gate_send.at[t], gate_recv.at[t, source], (f, z)).wait_recv()

    def z_first(t):
        @pl.when(z > 0)
        def _():
            pass_on(t, z, z - 1)

        @pl.when(z < nz - 1)
        def _():
            pass_on(t, z, z + 1)

    def z_hop(t, distance):
        @pl.when(z >= distance)
        def _():
            arrived(t, z - distance)

            @pl.when(z < nz - 1)
            def _():
                pass_on(t, z - distance, z + 1)

        @pl.when(z + distance < nz)
        def _():
            arrived(t, z + distance)

            @pl.when(z > 0)
            def _():
                pass_on(t, z + distance, z - 1)

    def rows_of(owner, t, start, size):
        return w_ref.at[t, pl.ds(pl.multiple_of(owner * line + start, shard), size)]

    def to_core(t, owner, start, size):
        remote(rows_of(owner, t, start, size), core_send.at[t], core_recv.at[t], (fc, z)).start()

    def line_done(t):
        mine = rows_of(f, t, 0, line)
        remote(mine, send_sem.at[t], x_recv.at[t], (fx, z)).start()
        remote(mine, send_sem.at[t], y_recv.at[t], (fy, z)).start()
        to_core(t, f, 0, line)

        @pl.when(t < gate_steps)
        def _():
            for source in range(nz):
                @pl.when(z != source)
                def _():
                    remote(
                        gate_of(t, source), gate_core_send.at[t], gate_core_recv.at[t], (fc, z)
                    ).start()

    def gate_done(t):
        @pl.when(t < gate_steps)
        def _():
            others = table_ref.at[pl.ds(0, (nz - 1) * piece)]
            pltpu.make_async_copy(others, others, gate_core_recv.at[t]).wait()

    def sides_done(t):
        from_x = rows_of(fx, t, 0, line)
        remote(from_x, send_sem.at[t], x_recv.at[t], (fx, z)).wait_recv()
        remote(rows_of(fx, t, 0, half), send_sem.at[t], a_recv.at[t], (fy, z)).start()
        to_core(t, fx, 0, line)
        from_y = rows_of(fy, t, 0, line)
        remote(from_y, send_sem.at[t], y_recv.at[t], (fy, z)).wait_recv()
        remote(rows_of(fy, t, half, half), send_sem.at[t], b_recv.at[t], (fx, z)).start()
        to_core(t, fy, 0, line)

    def corner_done(t):
        remote(rows_of(fd, t, 0, half), send_sem.at[t], a_recv.at[t], (fy, z)).wait_recv()
        to_core(t, fd, 0, half)
        remote(rows_of(fd, t, half, half), send_sem.at[t], b_recv.at[t], (fx, z)).wait_recv()
        to_core(t, fd, half, half)

    def multiply(t):
        whole = w_ref.at[t, pl.ds(0, 4 * line)]
        pltpu.make_async_copy(whole, whole, core_recv.at[t]).wait()
        blocks = normed_ref.shape[0] // 256
        column = pl.ds(pl.multiple_of((t % split) * LANES, LANES), LANES)

        def body(i, _):
            at = pl.ds(pl.multiple_of(i * 256, 256), 256)
            product = jnp.dot(normed_ref[at, :], w_ref[t], preferred_element_type=jnp.float32)

            @pl.when(t < split)
            def _():
                rec_ref[at, column] = product.astype(jnp.bfloat16)

            @pl.when(t >= split)
            def _():
                chunk = jnp.maximum(t - split, 0)
                state = b_ref[chunk, at, :] + a_ref[chunk, at, :] * start_ref[0:1, column]
                out_ref[at, column] = (state * jax.nn.gelu(product, approximate=True)).astype(out_ref.dtype)

            return 0

        lax.fori_loop(0, blocks, body, 0)

    def columns(h):
        return pl.ds(pl.multiple_of(h * channels, channels), channels)

    def tail_copy(h, source_rows, device):
        return pltpu.make_async_remote_copy(
            src_ref=rec_ref.at[pl.ds(source_rows, lead), columns(h)],
            dst_ref=before_ref.at[:, columns(h)],
            send_sem=tail_send.at[h], recv_sem=tail_recv.at[h],
            device_id=device, device_id_type=MESH,
        )

    def carry_copy(h, device):
        return pltpu.make_async_remote_copy(
            src_ref=carry_ref.at[:, columns(h)], dst_ref=start_ref.at[:, columns(h)],
            send_sem=carry_send.at[h], recv_sem=carry_recv.at[h],
            device_id=device, device_id_type=MESH,
        )

    def send_tail(h):
        @pl.when(z < nz - 1)
        def _():
            tail_copy(h, rows - lead, (f, z + 1)).start()

    def scan(h):
        @pl.when(z > 0)
        def _():
            tail_copy(h, rows - lead, (f, z)).wait_recv()

        cols = columns(h)
        padded_ref[pl.ds(0, lead), :] = before_ref[:, cols].astype(jnp.float32)
        padded_ref[pl.ds(lead, rows), :] = rec_ref[:, cols].astype(jnp.float32)
        conv_sum = jnp.zeros((rows, channels), jnp.float32) + bias_ref[:, cols]
        for tap in range(taps):
            conv_sum = conv_sum + weight_ref[tap : tap + 1, cols] * padded_ref[pl.ds(lead - tap, rows), :]
        conv_out = conv_sum.astype(jnp.bfloat16)
        gates = jnp.dot(conv_out, table_ref[cols, :], preferred_element_type=jnp.float32)
        input_gate = jax.nn.sigmoid(gates[:, :channels] + gate_bias_ref[0:1, cols])
        recur_gate = jax.nn.sigmoid(gates[:, channels:] + gate_bias_ref[1:2, cols])
        param = decay_ref[:, cols]
        softplus = jnp.maximum(param, 0.0) + jnp.log1p(jnp.exp(-jnp.abs(param)))
        log_decay = -8.0 * softplus * recur_gate
        decay = jnp.exp(log_decay)
        lost = -jnp.tanh(log_decay) * (decay * decay + 1.0)
        driven = jnp.sqrt(lost) * input_gate * conv_out.astype(jnp.float32)
        for j in range(pieces):
            a_ref[h * pieces + j] = decay[:, j * LANES : (j + 1) * LANES]
            b_ref[h * pieces + j] = driven[:, j * LANES : (j + 1) * LANES]

        lanes = 8
        length = rows // lanes

        def body(i, carry):
            at = pl.ds(i, lanes, stride=length)
            after = []
            for j in range(pieces):
                product, state = carry[j]
                decay_now = a_ref[h * pieces + j, at, :]
                product = product * decay_now
                state = decay_now * state + b_ref[h * pieces + j, at, :]
                a_ref[h * pieces + j, at, :] = product
                b_ref[h * pieces + j, at, :] = state
                after.append((product, state))
            return tuple(after)

        fresh = (jnp.ones((lanes, LANES), jnp.float32), jnp.zeros((lanes, LANES), jnp.float32))
        totals = lax.fori_loop(0, length, body, (fresh,) * pieces, unroll=8)
        for j in range(pieces):
            product, state = totals[j]
            start = jnp.zeros((1, LANES), jnp.float32)
            prefix = jnp.ones((1, LANES), jnp.float32)
            for i in range(lanes):
                at = pl.ds(i * length, length)
                within = a_ref[h * pieces + j, at, :]
                b_ref[h * pieces + j, at, :] = b_ref[h * pieces + j, at, :] + within * start
                a_ref[h * pieces + j, at, :] = within * prefix
                start = product[i : i + 1, :] * start + state[i : i + 1, :]
                prefix = prefix * product[i : i + 1, :]
            col = pl.ds(pl.multiple_of((h * pieces + j) * LANES, LANES), LANES)
            end_ref[0:1, col] = prefix
            end_ref[1:2, col] = start

    def make_carry(h):
        cols = columns(h)

        @pl.when(z > 0)
        def _():
            carry_copy(h, (f, z)).wait_recv()

        @pl.when(z < nz - 1)
        def _():
            end = end_ref[0:1, cols] * start_ref[0:1, cols] + end_ref[1:2, cols]
            carry_ref[:, cols] = jnp.broadcast_to(end, (carry_ref.shape[0], channels))

    def send_carry(h):
        @pl.when(z < nz - 1)
        def _():
            carry_copy(h, (f, z + 1)).start()

    @pl.when(z == 0)
    def _():
        before_ref[...] = jnp.zeros_like(before_ref)
        start_ref[...] = jnp.zeros_like(start_ref)

    stages = [z_first]
    for distance in range(1, nz):
        stages.append(functools.partial(z_hop, distance=distance))
    stages += [line_done, sides_done, corner_done, gate_done, multiply]
    lags = list(range(nz)) + [nz - 1, nz + 1, nz + 2, nz + 1, nz + 3]
    scan_at = gate_steps + nz

    def on_head(s, first, stage):
        @pl.when((s >= first) & (s < first + pieces * heads) & ((s - first) % pieces == 0))
        def _():
            stage((s - first) // pieces)

    def step(s, _):
        for stage, lag in zip(stages[:-1], lags[:-1]):
            @pl.when((s >= lag) & (s < chunks + lag))
            def _():
                stage(s - lag)

        on_head(s, scan_at + 2 + 2 * z, send_carry)
        on_head(s, lags[-1] + pieces, send_tail)

        @pl.when(s == 0)
        def _():
            normalise(tokens_ref, gain_ref, normed_ref)

        on_head(s, scan_at + 1 + 2 * z, make_carry)

        @pl.when((s >= lags[-1]) & (s < chunks + lags[-1]))
        def _():
            multiply(s - lags[-1])

        on_head(s, scan_at, scan)
        return 0

    lax.fori_loop(0, chunks + lags[-1], step, 0)

    def drain(t, _):
        for k in range(nz):
            shards_sent = (k + 1 if k < nz - 1 else 0) + (nz - k if k > 0 else 0)

            @pl.when(z == k)
            def _():
                sent = w_ref.at[t, pl.ds(0, shards_sent * shard + 3 * line)]
                pltpu.make_async_copy(sent, sent, send_sem.at[t]).wait()

                @pl.when(t < gate_steps)
                def _():
                    sent_gate = table_ref.at[pl.ds(0, shards_sent * piece)]
                    pltpu.make_async_copy(sent_gate, sent_gate, gate_send.at[t]).wait()

        whole = w_ref.at[t, pl.ds(0, 4 * line)]
        pltpu.make_async_copy(whole, whole, core_send.at[t]).wait()

        @pl.when(t < gate_steps)
        def _():
            others = table_ref.at[pl.ds(0, (nz - 1) * piece)]
            pltpu.make_async_copy(others, others, gate_core_send.at[t]).wait()

        @pl.when((t < heads) & (z < nz - 1))
        def _():
            tail_copy(t, rows - lead, (f, z)).wait_send()
            carry_copy(t, (f, z)).wait_send()

        return 0

    lax.fori_loop(0, chunks, drain, 0)


def fused_branch(
    nz, tokens, norm_gain, lru_proj, gelu_proj, conv_weight, conv_bias, gate_weights, gate_bias,
    decay_param,
):
    rows, width = tokens.shape
    inner = lru_proj.shape[1]
    chunks = 2 * inner // LANES
    channels = gate_weights.shape[1] // 2
    heads = inner // channels
    vmem = pl.BlockSpec(memory_space=pltpu.VMEM)
    any_ = pl.BlockSpec(memory_space=pl.ANY)
    dma = pltpu.SemaphoreType.DMA
    f32, bf16 = jnp.float32, jnp.bfloat16
    lead = 16
    return pl.pallas_call(
        functools.partial(branch_kernel, nz),
        out_shape=jax.ShapeDtypeStruct((rows, inner), bf16),
        in_specs=[vmem, vmem, any_, any_, any_, vmem, vmem, vmem, vmem],
        out_specs=vmem,
        scratch_shapes=[
            pltpu.VMEM((chunks, width, LANES), bf16),
            pltpu.VMEM((rows, width), bf16),
            pltpu.VMEM((rows, inner), bf16),
            pltpu.VMEM((gate_weights.shape[0] * nz, 2 * channels), bf16),
            pltpu.VMEM((lead, inner), bf16),
            pltpu.VMEM((lead + rows, channels), f32),
            pltpu.VMEM((chunks // 2, rows, LANES), f32),
            pltpu.VMEM((chunks // 2, rows, LANES), f32),
            pltpu.VMEM((8, inner), f32), pltpu.VMEM((8, inner), f32), pltpu.VMEM((8, inner), f32),
            dma((2,)), dma((chunks,)), dma((chunks,)), dma((chunks // 4,)), dma((chunks // 4,)),
            dma((heads,)), dma((heads,)),
            dma((chunks, nz)), dma((chunks // 4, nz)), dma((chunks // 4,)),
            dma((chunks,)), dma((chunks,)), dma((chunks,)), dma((chunks,)), dma((chunks,)),
            dma((heads,)), dma((heads,)),
        ],
        compiler_params=pltpu.CompilerParams(
            collective_id=0, has_side_effects=True, vmem_limit_bytes=VMEM_BYTES
        ),
    )(
        tokens, norm_gain.reshape(1, width), lru_proj, gelu_proj, gate_weights, conv_weight,
        conv_bias.reshape(1, inner), gate_bias, decay_param.reshape(1, inner),
    )


def scan_kernel(
    rec_ref, before_ref, weight_ref, bias_ref, table_ref, gate_bias_ref, decay_ref,
    state_ref, cumulative_ref, end_ref, padded_ref, a_ref, b_ref,
):
    rows, channels = rec_ref.shape
    taps = weight_ref.shape[0]
    lead = before_ref.shape[0]
    padded_ref[pl.ds(0, lead), :] = before_ref[...].astype(jnp.float32)
    padded_ref[pl.ds(lead, rows), :] = rec_ref[...].astype(jnp.float32)
    conv_sum = jnp.zeros((rows, channels), jnp.float32) + bias_ref[...]
    for tap in range(taps):
        conv_sum = conv_sum + weight_ref[tap : tap + 1, :] * padded_ref[pl.ds(lead - tap, rows), :]
    conv_out = conv_sum.astype(jnp.bfloat16)
    gates = jnp.dot(conv_out, table_ref[...], preferred_element_type=jnp.float32)
    input_gate = jax.nn.sigmoid(gates[:, :channels] + gate_bias_ref[0:1, :])
    recur_gate = jax.nn.sigmoid(gates[:, channels:] + gate_bias_ref[1:2, :])
    param = decay_ref[...]
    softplus = jnp.maximum(param, 0.0) + jnp.log1p(jnp.exp(-jnp.abs(param)))
    log_decay = -8.0 * softplus * recur_gate
    decay = jnp.exp(log_decay)
    lost = -jnp.tanh(log_decay) * (decay * decay + 1.0)
    driven = jnp.sqrt(lost) * input_gate * conv_out.astype(jnp.float32)
    parts = channels // LANES
    for j in range(parts):
        a_ref[j] = decay[:, j * LANES : (j + 1) * LANES]
        b_ref[j] = driven[:, j * LANES : (j + 1) * LANES]

    lanes = 8
    length = rows // lanes

    def body(i, carry):
        at = pl.ds(i, lanes, stride=length)
        after = []
        for j in range(parts):
            product, state = carry[j]
            decay_now = a_ref[j, at, :]
            product = product * decay_now
            state = decay_now * state + b_ref[j, at, :]
            a_ref[j, at, :] = product
            b_ref[j, at, :] = state
            after.append((product, state))
        return tuple(after)

    fresh = (jnp.ones((lanes, LANES), jnp.float32), jnp.zeros((lanes, LANES), jnp.float32))
    totals = lax.fori_loop(0, length, body, (fresh,) * parts, unroll=8)
    for j in range(parts):
        product, state = totals[j]
        cols = slice(j * LANES, (j + 1) * LANES)
        start = jnp.zeros((1, LANES), jnp.float32)
        prefix = jnp.ones((1, LANES), jnp.float32)
        for i in range(lanes):
            at = pl.ds(i * length, length)
            within = a_ref[j, at, :]
            state_ref[at, cols] = b_ref[j, at, :] + within * start
            cumulative_ref[at, cols] = within * prefix
            start = product[i : i + 1, :] * start + state[i : i + 1, :]
            prefix = prefix * product[i : i + 1, :]
        end_ref[0:1, cols] = prefix
        end_ref[1:2, cols] = start


def local_scan(rec, before, conv_weight, conv_bias, table, gate_bias, decay_param):
    rows, inner = rec.shape
    width = table.shape[1] // 2
    lead = before.shape[0]

    def columns(height):
        return pl.BlockSpec((height, width), lambda h: (0, h))

    return pl.pallas_call(
        scan_kernel,
        grid=(inner // width,),
        out_shape=(
            jax.ShapeDtypeStruct((rows, inner), jnp.float32),
            jax.ShapeDtypeStruct((rows, inner), jnp.float32),
            jax.ShapeDtypeStruct((2, inner), jnp.float32),
        ),
        in_specs=[
            columns(rows), columns(lead), columns(conv_weight.shape[0]), columns(1),
            pl.BlockSpec((width, 2 * width), lambda h: (h, 0)), columns(2), columns(1),
        ],
        out_specs=(columns(rows), columns(rows), columns(2)),
        scratch_shapes=[
            pltpu.VMEM((rows + lead, width), jnp.float32),
            pltpu.VMEM((width // LANES, rows, LANES), jnp.float32),
            pltpu.VMEM((width // LANES, rows, LANES), jnp.float32),
        ],
    )(
        rec, before, conv_weight, conv_bias.reshape(1, inner), table, gate_bias,
        decay_param.reshape(1, inner),
    )


def shards(
    nz, paired, tokens, norm_gain, lru_proj, gelu_proj, conv_weight, conv_bias, gate_weights,
    gate_bias, decay_param,
):
    seq_count, tok_rows, width = tokens.shape
    inner = lru_proj.shape[1]
    taps = conv_weight.shape[0]
    if paired:
        out = fused_branch(
            nz, tokens.reshape(tok_rows, width), norm_gain, lru_proj, gelu_proj, conv_weight,
            conv_bias, gate_weights, gate_bias, decay_param,
        )
        return out.reshape(seq_count, tok_rows, inner)
    flat = tokens.reshape(tok_rows, width).astype(jnp.float32)
    mean_square = jnp.mean(flat * flat, axis=-1, keepdims=True)
    normed = (flat * lax.rsqrt(mean_square + 1e-06) * norm_gain).astype(jnp.bfloat16)
    every = [
        lax.all_gather(w, ("fsdp", "seq"), axis=0, tiled=True) for w in (lru_proj, gelu_proj)
    ]
    rec = jnp.dot(normed, every[0], preferred_element_type=jnp.float32).astype(jnp.bfloat16)
    act = jnp.dot(normed, every[1], preferred_element_type=jnp.float32)
    table = lax.all_gather(gate_weights, "seq", axis=0, tiled=True)
    lead = 8
    before = lax.ppermute(
        rec[tok_rows - lead :, :], "seq", [(i, i + 1) for i in range(nz - 1)]
    )
    local, cumulative, ends = local_scan(
        rec, before, conv_weight, conv_bias, table, gate_bias, decay_param
    )
    every_end = lax.all_gather(ends, "seq")
    position = lax.axis_index("seq")
    start = jnp.zeros((inner,), jnp.float32)
    for k in range(nz - 1):
        start = jnp.where(k < position, every_end[k, 0] * start + every_end[k, 1], start)
    gelu = jax.nn.gelu(act, approximate=True)
    out = ((local + cumulative * start) * gelu).astype(jnp.bfloat16)
    return out.reshape(seq_count, tok_rows, inner)


def solution(mesh):
    placed = (
        P("fsdp", "seq", None), P(), P(("fsdp", "seq"), None), P(("fsdp", "seq"), None), P(), P(),
        P("seq", None), P(), P(),
    )
    nz = mesh.shape["seq"]
    paired = mesh.shape["fsdp"] == 8 and 1 < nz <= 5
    return jax.shard_map(
        functools.partial(shards, nz, paired), mesh=mesh, in_specs=placed,
        out_specs=P("fsdp", "seq", None), check_vma=False,
    )
```

```python
import functools

import jax
import jax.numpy as jnp
from jax import lax
from jax.experimental import pallas as pl
from jax.experimental.pallas import tpu as pltpu
from jax.sharding import PartitionSpec as P

MESH = pl.DeviceIdType.MESH
LANES = 128
VMEM_BYTES = 66_000_000


def normalise(tokens_ref, gain_ref, normed_ref, part, parts):
    rows = 32

    def body(i, _):
        at = pl.ds(pl.multiple_of(i * rows, rows), rows)
        values = tokens_ref[at, :].astype(jnp.float32)
        mean_square = jnp.mean(values * values, axis=-1, keepdims=True)
        normed_ref[at, :] = (values * lax.rsqrt(mean_square + 1e-06) * gain_ref[...]).astype(jnp.bfloat16)
        return 0

    blocks = tokens_ref.shape[0] // rows // parts
    lax.fori_loop(part * blocks, (part + 1) * blocks, body, 0)


def branch_kernel(
    nz,
    tokens_ref, gain_ref, lru_ref, gelu_ref, gate_ref,
    weight_ref, bias_ref, gate_bias_ref, decay_ref,
    out_ref,
    w_ref, normed_ref, rec_ref, table_ref, before_ref, padded_ref, a_ref, b_ref,
    end_ref, carry_ref, start_ref,
    own_sem, send_sem, core_send, gate_send, gate_core_send, tail_send, carry_send,
    z_recv, gate_recv, gate_core_recv, x_recv, y_recv, a_recv, b_recv, core_recv,
    tail_recv, carry_recv,
):
    f = lax.axis_index("fsdp")
    z = lax.axis_index("seq")
    c, x, y = f % 2, (f // 2) % 2, f // 4
    fx, fy, fc = f + 2 - 4 * x, f + 4 - 8 * y, f + 1 - 2 * c
    fd = fx + 4 - 8 * y
    shard = lru_ref.shape[0]
    line = shard * nz
    half = line // 2
    chunks = w_ref.shape[0]
    split = chunks // 2
    gate_rows = gate_ref.shape[0]
    gate_steps = split // 2
    piece = gate_rows // 2 // gate_steps
    rows = normed_ref.shape[0]
    channels = table_ref.shape[1] // 2
    heads = rec_ref.shape[1] // channels
    pieces = channels // LANES
    taps = weight_ref.shape[0]
    lead = before_ref.shape[0]

    def remote(src, send, recv, device):
        return pltpu.make_async_remote_copy(
            src_ref=src, dst_ref=src, send_sem=send, recv_sem=recv,
            device_id=device, device_id_type=MESH,
        )

    own = pl.ds(pl.multiple_of((f * nz + z) * shard, shard), shard)
    for t in range(chunks):
        src = lru_ref if t < split else gelu_ref
        cols = pl.ds((t % split) * LANES, LANES)
        pltpu.make_async_copy(src.at[:, cols], w_ref.at[t, own], own_sem.at[0]).start()
    own_gate = pl.ds(pl.multiple_of(z * gate_rows, gate_rows), gate_rows)
    gate_copy = pltpu.make_async_copy(gate_ref, table_ref.at[own_gate], own_sem.at[1])
    gate_copy.start()

    barrier = pltpu.get_barrier_semaphore()
    for device in ((fx, z), (fy, z), (fc, z)):
        pl.semaphore_signal(barrier, inc=1, device_id=device, device_id_type=MESH)

    @pl.when(z > 0)
    def _():
        pl.semaphore_signal(barrier, inc=1, device_id=(f, z - 1), device_id_type=MESH)

    @pl.when(z < nz - 1)
    def _():
        pl.semaphore_signal(barrier, inc=1, device_id=(f, z + 1), device_id_type=MESH)

    for k in range(nz):
        @pl.when(z == k)
        def _():
            pl.semaphore_wait(barrier, 3 + int(k > 0) + int(k < nz - 1))

    pltpu.make_async_copy(w_ref.at[:, own], w_ref.at[:, own], own_sem.at[0]).wait()
    gate_copy.wait()

    def shard_of(t, source):
        at = pl.ds(pl.multiple_of((f * nz + source) * shard, shard), shard)
        return w_ref.at[t, at]

    def gate_of(t, source):
        first = source * gate_rows + c * (gate_rows // 2) + t * piece
        return table_ref.at[pl.ds(pl.multiple_of(first, piece), piece)]

    def pass_on(t, source, target):
        remote(shard_of(t, source), send_sem.at[t], z_recv.at[t, source], (f, target)).start()

        @pl.when(t < gate_steps)
        def _():
            remote(gate_of(t, source), gate_send.at[t], gate_recv.at[t, source], (f, target)).start()

    def arrived(t, source):
        remote(shard_of(t, source), send_sem.at[t], z_recv.at[t, source], (f, z)).wait_recv()

        @pl.when(t < gate_steps)
        def _():
            remote(gate_of(t, source), gate_send.at[t], gate_recv.at[t, source], (f, z)).wait_recv()

    def z_first(t):
        @pl.when(z > 0)
        def _():
            pass_on(t, z, z - 1)

        @pl.when(z < nz - 1)
        def _():
            pass_on(t, z, z + 1)

    def z_hop(t, distance):
        @pl.when(z >= distance)
        def _():
            arrived(t, z - distance)

            @pl.when(z < nz - 1)
            def _():
                pass_on(t, z - distance, z + 1)

        @pl.when(z + distance < nz)
        def _():
            arrived(t, z + distance)

            @pl.when(z > 0)
            def _():
                pass_on(t, z + distance, z - 1)

    def rows_of(owner, t, start, size):
        return w_ref.at[t, pl.ds(pl.multiple_of(owner * line + start, shard), size)]

    def to_core(t, owner, start, size):
        remote(rows_of(owner, t, start, size), core_send.at[t], core_recv.at[t], (fc, z)).start()

    def line_done(t):
        mine = rows_of(f, t, 0, line)
        remote(mine, send_sem.at[t], x_recv.at[t], (fx, z)).start()
        remote(mine, send_sem.at[t], y_recv.at[t], (fy, z)).start()
        to_core(t, f, 0, line)

        @pl.when(t < gate_steps)
        def _():
            for source in range(nz):
                @pl.when(z != source)
                def _():
                    remote(
                        gate_of(t, source), gate_core_send.at[t], gate_core_recv.at[t], (fc, z)
                    ).start()

    def gate_done(t):
        @pl.when(t < gate_steps)
        def _():
            others = table_ref.at[pl.ds(0, (nz - 1) * piece)]
            pltpu.make_async_copy(others, others, gate_core_recv.at[t]).wait()

    def sides_done(t):
        from_x = rows_of(fx, t, 0, line)
        remote(from_x, send_sem.at[t], x_recv.at[t], (fx, z)).wait_recv()
        remote(rows_of(fx, t, 0, half), send_sem.at[t], a_recv.at[t], (fy, z)).start()
        to_core(t, fx, 0, line)
        from_y = rows_of(fy, t, 0, line)
        remote(from_y, send_sem.at[t], y_recv.at[t], (fy, z)).wait_recv()
        remote(rows_of(fy, t, half, half), send_sem.at[t], b_recv.at[t], (fx, z)).start()
        to_core(t, fy, 0, line)

    def corner_done(t):
        remote(rows_of(fd, t, 0, half), send_sem.at[t], a_recv.at[t], (fy, z)).wait_recv()
        to_core(t, fd, 0, half)
        remote(rows_of(fd, t, half, half), send_sem.at[t], b_recv.at[t], (fx, z)).wait_recv()
        to_core(t, fd, half, half)

    def multiply(t):
        whole = w_ref.at[t, pl.ds(0, 4 * line)]
        pltpu.make_async_copy(whole, whole, core_recv.at[t]).wait()
        blocks = normed_ref.shape[0] // 256
        column = pl.ds(pl.multiple_of((t % split) * LANES, LANES), LANES)

        def body(i, _):
            at = pl.ds(pl.multiple_of(i * 256, 256), 256)
            product = jnp.dot(normed_ref[at, :], w_ref[t], preferred_element_type=jnp.float32)

            @pl.when(t < split)
            def _():
                rec_ref[at, column] = product.astype(jnp.bfloat16)

            @pl.when(t >= split)
            def _():
                chunk = jnp.maximum(t - split, 0)
                state = b_ref[chunk, at, :] + a_ref[chunk, at, :] * start_ref[0:1, column]
                out_ref[at, column] = (state * jax.nn.gelu(product, approximate=True)).astype(out_ref.dtype)

            return 0

        lax.fori_loop(0, blocks, body, 0)

    def columns(h):
        return pl.ds(pl.multiple_of(h * channels, channels), channels)

    def tail_copy(h, source_rows, device):
        return pltpu.make_async_remote_copy(
            src_ref=rec_ref.at[pl.ds(source_rows, lead), columns(h)],
            dst_ref=before_ref.at[:, columns(h)],
            send_sem=tail_send.at[h], recv_sem=tail_recv.at[h],
            device_id=device, device_id_type=MESH,
        )

    def carry_copy(h, device):
        return pltpu.make_async_remote_copy(
            src_ref=carry_ref.at[:, columns(h)], dst_ref=start_ref.at[:, columns(h)],
            send_sem=carry_send.at[h], recv_sem=carry_recv.at[h],
            device_id=device, device_id_type=MESH,
        )

    def send_tail(h):
        @pl.when(z < nz - 1)
        def _():
            tail_copy(h, rows - lead, (f, z + 1)).start()

    def scan(h):
        @pl.when(z > 0)
        def _():
            tail_copy(h, rows - lead, (f, z)).wait_recv()

        cols = columns(h)
        padded_ref[pl.ds(0, lead), :] = before_ref[:, cols].astype(jnp.float32)
        padded_ref[pl.ds(lead, rows), :] = rec_ref[:, cols].astype(jnp.float32)
        conv_sum = jnp.zeros((rows, channels), jnp.float32) + bias_ref[:, cols]
        for tap in range(taps):
            conv_sum = conv_sum + weight_ref[tap : tap + 1, cols] * padded_ref[pl.ds(lead - tap, rows), :]
        conv_out = conv_sum.astype(jnp.bfloat16)
        gates = jnp.dot(conv_out, table_ref[cols, :], preferred_element_type=jnp.float32)
        input_gate = jax.nn.sigmoid(gates[:, :channels] + gate_bias_ref[0:1, cols])
        recur_gate = jax.nn.sigmoid(gates[:, channels:] + gate_bias_ref[1:2, cols])
        param = decay_ref[:, cols]
        softplus = jnp.maximum(param, 0.0) + jnp.log1p(jnp.exp(-jnp.abs(param)))
        log_decay = -8.0 * softplus * recur_gate
        decay = jnp.exp(log_decay)
        lost = -jnp.tanh(log_decay) * (decay * decay + 1.0)
        driven = jnp.sqrt(lost) * input_gate * conv_out.astype(jnp.float32)
        for j in range(pieces):
            a_ref[h * pieces + j] = decay[:, j * LANES : (j + 1) * LANES]
            b_ref[h * pieces + j] = driven[:, j * LANES : (j + 1) * LANES]

        lanes = 8
        length = rows // lanes

        def body(i, carry):
            at = pl.ds(i, lanes, stride=length)
            after = []
            for j in range(pieces):
                product, state = carry[j]
                decay_now = a_ref[h * pieces + j, at, :]
                product = product * decay_now
                state = decay_now * state + b_ref[h * pieces + j, at, :]
                a_ref[h * pieces + j, at, :] = product
                b_ref[h * pieces + j, at, :] = state
                after.append((product, state))
            return tuple(after)

        fresh = (jnp.ones((lanes, LANES), jnp.float32), jnp.zeros((lanes, LANES), jnp.float32))
        totals = lax.fori_loop(0, length, body, (fresh,) * pieces, unroll=8)
        for j in range(pieces):
            product, state = totals[j]
            start = jnp.zeros((1, LANES), jnp.float32)
            prefix = jnp.ones((1, LANES), jnp.float32)
            for i in range(lanes):
                at = pl.ds(i * length, length)
                within = a_ref[h * pieces + j, at, :]
                b_ref[h * pieces + j, at, :] = b_ref[h * pieces + j, at, :] + within * start
                a_ref[h * pieces + j, at, :] = within * prefix
                start = product[i : i + 1, :] * start + state[i : i + 1, :]
                prefix = prefix * product[i : i + 1, :]
            col = pl.ds(pl.multiple_of((h * pieces + j) * LANES, LANES), LANES)
            end_ref[0:1, col] = prefix
            end_ref[1:2, col] = start

    def make_carry(h):
        cols = columns(h)

        @pl.when(z > 0)
        def _():
            carry_copy(h, (f, z)).wait_recv()

        @pl.when(z < nz - 1)
        def _():
            end = end_ref[0:1, cols] * start_ref[0:1, cols] + end_ref[1:2, cols]
            carry_ref[:, cols] = jnp.broadcast_to(end, (carry_ref.shape[0], channels))

    def send_carry(h):
        @pl.when(z < nz - 1)
        def _():
            carry_copy(h, (f, z + 1)).start()

    @pl.when(z == 0)
    def _():
        before_ref[...] = jnp.zeros_like(before_ref)
        start_ref[...] = jnp.zeros_like(start_ref)

    stages = [z_first]
    for distance in range(1, nz):
        stages.append(functools.partial(z_hop, distance=distance))
    stages += [line_done, sides_done, corner_done, gate_done, multiply]
    lags = list(range(nz)) + [nz - 1, nz, nz + 1, nz + 1, nz + 2]
    scan_at = gate_steps + nz

    def on_head(s, first, stage):
        @pl.when((s >= first) & (s < first + pieces * heads) & ((s - first) % pieces == 0))
        def _():
            stage((s - first) // pieces)

    def step(s, _):
        for stage, lag in zip(stages[:-1], lags[:-1]):
            @pl.when((s >= lag) & (s < chunks + lag))
            def _():
                stage(s - lag)

        on_head(s, scan_at + 2 + 2 * z, send_carry)
        on_head(s, nz + 2 + pieces, send_tail)

        @pl.when(s < 4)
        def _():
            normalise(tokens_ref, gain_ref, normed_ref, s, 4)

        on_head(s, scan_at + 1 + 2 * z, make_carry)

        @pl.when((s >= lags[-1]) & (s < chunks + lags[-1]))
        def _():
            multiply(s - lags[-1])

        on_head(s, scan_at, scan)
        return 0

    lax.fori_loop(0, chunks + lags[-1], step, 0)

    def drain(t, _):
        for k in range(nz):
            shards_sent = (k + 1 if k < nz - 1 else 0) + (nz - k if k > 0 else 0)

            @pl.when(z == k)
            def _():
                sent = w_ref.at[t, pl.ds(0, shards_sent * shard + 3 * line)]
                pltpu.make_async_copy(sent, sent, send_sem.at[t]).wait()

                @pl.when(t < gate_steps)
                def _():
                    sent_gate = table_ref.at[pl.ds(0, shards_sent * piece)]
                    pltpu.make_async_copy(sent_gate, sent_gate, gate_send.at[t]).wait()

        whole = w_ref.at[t, pl.ds(0, 4 * line)]
        pltpu.make_async_copy(whole, whole, core_send.at[t]).wait()

        @pl.when(t < gate_steps)
        def _():
            others = table_ref.at[pl.ds(0, (nz - 1) * piece)]
            pltpu.make_async_copy(others, others, gate_core_send.at[t]).wait()

        @pl.when((t < heads) & (z < nz - 1))
        def _():
            tail_copy(t, rows - lead, (f, z)).wait_send()
            carry_copy(t, (f, z)).wait_send()

        return 0

    lax.fori_loop(0, chunks, drain, 0)


def fused_branch(
    nz, tokens, norm_gain, lru_proj, gelu_proj, conv_weight, conv_bias, gate_weights, gate_bias,
    decay_param,
):
    rows, width = tokens.shape
    inner = lru_proj.shape[1]
    chunks = 2 * inner // LANES
    channels = gate_weights.shape[1] // 2
    heads = inner // channels
    vmem = pl.BlockSpec(memory_space=pltpu.VMEM)
    any_ = pl.BlockSpec(memory_space=pl.ANY)
    dma = pltpu.SemaphoreType.DMA
    f32, bf16 = jnp.float32, jnp.bfloat16
    lead = 16
    return pl.pallas_call(
        functools.partial(branch_kernel, nz),
        out_shape=jax.ShapeDtypeStruct((rows, inner), bf16),
        in_specs=[vmem, vmem, any_, any_, any_, vmem, vmem, vmem, vmem],
        out_specs=vmem,
        scratch_shapes=[
            pltpu.VMEM((chunks, width, LANES), bf16),
            pltpu.VMEM((rows, width), bf16),
            pltpu.VMEM((rows, inner), bf16),
            pltpu.VMEM((gate_weights.shape[0] * nz, 2 * channels), bf16),
            pltpu.VMEM((lead, inner), bf16),
            pltpu.VMEM((lead + rows, channels), f32),
            pltpu.VMEM((chunks // 2, rows, LANES), f32),
            pltpu.VMEM((chunks // 2, rows, LANES), f32),
            pltpu.VMEM((8, inner), f32), pltpu.VMEM((8, inner), f32), pltpu.VMEM((8, inner), f32),
            dma((2,)), dma((chunks,)), dma((chunks,)), dma((chunks // 4,)), dma((chunks // 4,)),
            dma((heads,)), dma((heads,)),
            dma((chunks, nz)), dma((chunks // 4, nz)), dma((chunks // 4,)),
            dma((chunks,)), dma((chunks,)), dma((chunks,)), dma((chunks,)), dma((chunks,)),
            dma((heads,)), dma((heads,)),
        ],
        compiler_params=pltpu.CompilerParams(
            collective_id=0, has_side_effects=True, vmem_limit_bytes=VMEM_BYTES
        ),
    )(
        tokens, norm_gain.reshape(1, width), lru_proj, gelu_proj, gate_weights, conv_weight,
        conv_bias.reshape(1, inner), gate_bias, decay_param.reshape(1, inner),
    )


def scan_kernel(
    rec_ref, before_ref, weight_ref, bias_ref, table_ref, gate_bias_ref, decay_ref,
    state_ref, cumulative_ref, end_ref, padded_ref, a_ref, b_ref,
):
    rows, channels = rec_ref.shape
    taps = weight_ref.shape[0]
    lead = before_ref.shape[0]
    padded_ref[pl.ds(0, lead), :] = before_ref[...].astype(jnp.float32)
    padded_ref[pl.ds(lead, rows), :] = rec_ref[...].astype(jnp.float32)
    conv_sum = jnp.zeros((rows, channels), jnp.float32) + bias_ref[...]
    for tap in range(taps):
        conv_sum = conv_sum + weight_ref[tap : tap + 1, :] * padded_ref[pl.ds(lead - tap, rows), :]
    conv_out = conv_sum.astype(jnp.bfloat16)
    gates = jnp.dot(conv_out, table_ref[...], preferred_element_type=jnp.float32)
    input_gate = jax.nn.sigmoid(gates[:, :channels] + gate_bias_ref[0:1, :])
    recur_gate = jax.nn.sigmoid(gates[:, channels:] + gate_bias_ref[1:2, :])
    param = decay_ref[...]
    softplus = jnp.maximum(param, 0.0) + jnp.log1p(jnp.exp(-jnp.abs(param)))
    log_decay = -8.0 * softplus * recur_gate
    decay = jnp.exp(log_decay)
    lost = -jnp.tanh(log_decay) * (decay * decay + 1.0)
    driven = jnp.sqrt(lost) * input_gate * conv_out.astype(jnp.float32)
    parts = channels // LANES
    for j in range(parts):
        a_ref[j] = decay[:, j * LANES : (j + 1) * LANES]
        b_ref[j] = driven[:, j * LANES : (j + 1) * LANES]

    lanes = 8
    length = rows // lanes

    def body(i, carry):
        at = pl.ds(i, lanes, stride=length)
        after = []
        for j in range(parts):
            product, state = carry[j]
            decay_now = a_ref[j, at, :]
            product = product * decay_now
            state = decay_now * state + b_ref[j, at, :]
            a_ref[j, at, :] = product
            b_ref[j, at, :] = state
            after.append((product, state))
        return tuple(after)

    fresh = (jnp.ones((lanes, LANES), jnp.float32), jnp.zeros((lanes, LANES), jnp.float32))
    totals = lax.fori_loop(0, length, body, (fresh,) * parts, unroll=8)
    for j in range(parts):
        product, state = totals[j]
        cols = slice(j * LANES, (j + 1) * LANES)
        start = jnp.zeros((1, LANES), jnp.float32)
        prefix = jnp.ones((1, LANES), jnp.float32)
        for i in range(lanes):
            at = pl.ds(i * length, length)
            within = a_ref[j, at, :]
            state_ref[at, cols] = b_ref[j, at, :] + within * start
            cumulative_ref[at, cols] = within * prefix
            start = product[i : i + 1, :] * start + state[i : i + 1, :]
            prefix = prefix * product[i : i + 1, :]
        end_ref[0:1, cols] = prefix
        end_ref[1:2, cols] = start


def local_scan(rec, before, conv_weight, conv_bias, table, gate_bias, decay_param):
    rows, inner = rec.shape
    width = table.shape[1] // 2
    lead = before.shape[0]

    def columns(height):
        return pl.BlockSpec((height, width), lambda h: (0, h))

    return pl.pallas_call(
        scan_kernel,
        grid=(inner // width,),
        out_shape=(
            jax.ShapeDtypeStruct((rows, inner), jnp.float32),
            jax.ShapeDtypeStruct((rows, inner), jnp.float32),
            jax.ShapeDtypeStruct((2, inner), jnp.float32),
        ),
        in_specs=[
            columns(rows), columns(lead), columns(conv_weight.shape[0]), columns(1),
            pl.BlockSpec((width, 2 * width), lambda h: (h, 0)), columns(2), columns(1),
        ],
        out_specs=(columns(rows), columns(rows), columns(2)),
        scratch_shapes=[
            pltpu.VMEM((rows + lead, width), jnp.float32),
            pltpu.VMEM((width // LANES, rows, LANES), jnp.float32),
            pltpu.VMEM((width // LANES, rows, LANES), jnp.float32),
        ],
    )(
        rec, before, conv_weight, conv_bias.reshape(1, inner), table, gate_bias,
        decay_param.reshape(1, inner),
    )


def shards(
    nz, paired, tokens, norm_gain, lru_proj, gelu_proj, conv_weight, conv_bias, gate_weights,
    gate_bias, decay_param,
):
    seq_count, tok_rows, width = tokens.shape
    inner = lru_proj.shape[1]
    taps = conv_weight.shape[0]
    if paired:
        out = fused_branch(
            nz, tokens.reshape(tok_rows, width), norm_gain, lru_proj, gelu_proj, conv_weight,
            conv_bias, gate_weights, gate_bias, decay_param,
        )
        return out.reshape(seq_count, tok_rows, inner)
    flat = tokens.reshape(tok_rows, width).astype(jnp.float32)
    mean_square = jnp.mean(flat * flat, axis=-1, keepdims=True)
    normed = (flat * lax.rsqrt(mean_square + 1e-06) * norm_gain).astype(jnp.bfloat16)
    every = [
        lax.all_gather(w, ("fsdp", "seq"), axis=0, tiled=True) for w in (lru_proj, gelu_proj)
    ]
    rec = jnp.dot(normed, every[0], preferred_element_type=jnp.float32).astype(jnp.bfloat16)
    act = jnp.dot(normed, every[1], preferred_element_type=jnp.float32)
    table = lax.all_gather(gate_weights, "seq", axis=0, tiled=True)
    lead = 8
    before = lax.ppermute(
        rec[tok_rows - lead :, :], "seq", [(i, i + 1) for i in range(nz - 1)]
    )
    local, cumulative, ends = local_scan(
        rec, before, conv_weight, conv_bias, table, gate_bias, decay_param
    )
    every_end = lax.all_gather(ends, "seq")
    position = lax.axis_index("seq")
    start = jnp.zeros((inner,), jnp.float32)
    for k in range(nz - 1):
        start = jnp.where(k < position, every_end[k, 0] * start + every_end[k, 1], start)
    gelu = jax.nn.gelu(act, approximate=True)
    out = ((local + cumulative * start) * gelu).astype(jnp.bfloat16)
    return out.reshape(seq_count, tok_rows, inner)


def solution(mesh):
    placed = (
        P("fsdp", "seq", None), P(), P(("fsdp", "seq"), None), P(("fsdp", "seq"), None), P(), P(),
        P("seq", None), P(), P(),
    )
    nz = mesh.shape["seq"]
    paired = mesh.shape["fsdp"] == 8 and 1 < nz <= 5
    return jax.shard_map(
        functools.partial(shards, nz, paired), mesh=mesh, in_specs=placed,
        out_specs=P("fsdp", "seq", None), check_vma=False,
    )
```

```python
import functools

import jax
import jax.numpy as jnp
from jax import lax
from jax.experimental import pallas as pl
from jax.experimental.pallas import tpu as pltpu
from jax.sharding import PartitionSpec as P

MESH = pl.DeviceIdType.MESH
LANES = 128
VMEM_BYTES = 66_000_000


def normalise(tokens_ref, gain_ref, normed_ref, part, parts):
    rows = 32

    def body(i, _):
        at = pl.ds(pl.multiple_of(i * rows, rows), rows)
        values = tokens_ref[at, :].astype(jnp.float32)
        mean_square = jnp.mean(values * values, axis=-1, keepdims=True)
        normed_ref[at, :] = (values * lax.rsqrt(mean_square + 1e-06) * gain_ref[...]).astype(jnp.bfloat16)
        return 0

    blocks = tokens_ref.shape[0] // rows // parts
    lax.fori_loop(part * blocks, (part + 1) * blocks, body, 0)


def branch_kernel(
    nz,
    tokens_ref, gain_ref, lru_ref, gelu_ref, gate_ref,
    weight_ref, bias_ref, gate_bias_ref, decay_ref,
    out_ref,
    w_ref, normed_ref, rec_ref, table_ref, before_ref, padded_ref, a_ref, b_ref,
    end_ref, carry_ref, start_ref,
    own_sem, send_sem, core_send, gate_send, gate_core_send, tail_send, carry_send,
    z_recv, gate_recv, gate_core_recv, x_recv, y_recv, a_recv, b_recv, core_recv,
    tail_recv, carry_recv,
):
    f = lax.axis_index("fsdp")
    z = lax.axis_index("seq")
    c, x, y = f % 2, (f // 2) % 2, f // 4
    fx, fy, fc = f + 2 - 4 * x, f + 4 - 8 * y, f + 1 - 2 * c
    fd = fx + 4 - 8 * y
    shard = lru_ref.shape[0]
    line = shard * nz
    half = line // 2
    chunks = w_ref.shape[0]
    split = chunks // 2
    gate_rows = gate_ref.shape[0]
    gate_steps = split // 2
    piece = gate_rows // 2 // gate_steps
    rows = normed_ref.shape[0]
    channels = table_ref.shape[1] // 2
    heads = rec_ref.shape[1] // channels
    pieces = channels // LANES
    taps = weight_ref.shape[0]
    lead = before_ref.shape[0]

    def remote(src, send, recv, device):
        return pltpu.make_async_remote_copy(
            src_ref=src, dst_ref=src, send_sem=send, recv_sem=recv,
            device_id=device, device_id_type=MESH,
        )

    own = pl.ds(pl.multiple_of((f * nz + z) * shard, shard), shard)
    for t in range(chunks):
        src = lru_ref if t < split else gelu_ref
        cols = pl.ds((t % split) * LANES, LANES)
        pltpu.make_async_copy(src.at[:, cols], w_ref.at[t, own], own_sem.at[0]).start()
    own_gate = pl.ds(pl.multiple_of(z * gate_rows, gate_rows), gate_rows)
    gate_copy = pltpu.make_async_copy(gate_ref, table_ref.at[own_gate], own_sem.at[1])
    gate_copy.start()

    barrier = pltpu.get_barrier_semaphore()
    for device in ((fx, z), (fy, z), (fc, z)):
        pl.semaphore_signal(barrier, inc=1, device_id=device, device_id_type=MESH)

    @pl.when(z > 0)
    def _():
        pl.semaphore_signal(barrier, inc=1, device_id=(f, z - 1), device_id_type=MESH)

    @pl.when(z < nz - 1)
    def _():
        pl.semaphore_signal(barrier, inc=1, device_id=(f, z + 1), device_id_type=MESH)

    for k in range(nz):
        @pl.when(z == k)
        def _():
            pl.semaphore_wait(barrier, 3 + int(k > 0) + int(k < nz - 1))

    pltpu.make_async_copy(w_ref.at[:, own], w_ref.at[:, own], own_sem.at[0]).wait()
    gate_copy.wait()

    def shard_of(t, source):
        at = pl.ds(pl.multiple_of((f * nz + source) * shard, shard), shard)
        return w_ref.at[t, at]

    def gate_of(t, source):
        first = source * gate_rows + c * (gate_rows // 2) + t * piece
        return table_ref.at[pl.ds(pl.multiple_of(first, piece), piece)]

    def pass_on(t, source, target):
        remote(shard_of(t, source), send_sem.at[t], z_recv.at[t, source], (f, target)).start()

        @pl.when(t < gate_steps)
        def _():
            remote(gate_of(t, source), gate_send.at[t], gate_recv.at[t, source], (f, target)).start()

    def arrived(t, source):
        remote(shard_of(t, source), send_sem.at[t], z_recv.at[t, source], (f, z)).wait_recv()

        @pl.when(t < gate_steps)
        def _():
            remote(gate_of(t, source), gate_send.at[t], gate_recv.at[t, source], (f, z)).wait_recv()

    def z_first(t):
        @pl.when(z > 0)
        def _():
            pass_on(t, z, z - 1)

        @pl.when(z < nz - 1)
        def _():
            pass_on(t, z, z + 1)

    def z_hop(t, distance):
        @pl.when(z >= distance)
        def _():
            arrived(t, z - distance)

            @pl.when(z < nz - 1)
            def _():
                pass_on(t, z - distance, z + 1)

        @pl.when(z + distance < nz)
        def _():
            arrived(t, z + distance)

            @pl.when(z > 0)
            def _():
                pass_on(t, z + distance, z - 1)

    def rows_of(owner, t, start, size):
        return w_ref.at[t, pl.ds(pl.multiple_of(owner * line + start, shard), size)]

    def to_core(t, owner, start, size):
        remote(rows_of(owner, t, start, size), core_send.at[t], core_recv.at[t], (fc, z)).start()

    def line_done(t):
        mine = rows_of(f, t, 0, line)
        remote(mine, send_sem.at[t], x_recv.at[t], (fx, z)).start()
        remote(mine, send_sem.at[t], y_recv.at[t], (fy, z)).start()
        to_core(t, f, 0, line)

        @pl.when(t < gate_steps)
        def _():
            for source in range(nz):
                @pl.when(z != source)
                def _():
                    remote(
                        gate_of(t, source), gate_core_send.at[t], gate_core_recv.at[t], (fc, z)
                    ).start()

    def gate_done(t):
        @pl.when(t < gate_steps)
        def _():
            others = table_ref.at[pl.ds(0, (nz - 1) * piece)]
            pltpu.make_async_copy(others, others, gate_core_recv.at[t]).wait()

    def sides_done(t):
        from_x = rows_of(fx, t, 0, line)
        remote(from_x, send_sem.at[t], x_recv.at[t], (fx, z)).wait_recv()
        remote(rows_of(fx, t, 0, half), send_sem.at[t], a_recv.at[t], (fy, z)).start()
        to_core(t, fx, 0, line)
        from_y = rows_of(fy, t, 0, line)
        remote(from_y, send_sem.at[t], y_recv.at[t], (fy, z)).wait_recv()
        remote(rows_of(fy, t, half, half), send_sem.at[t], b_recv.at[t], (fx, z)).start()
        to_core(t, fy, 0, line)

    def corner_done(t):
        remote(rows_of(fd, t, 0, half), send_sem.at[t], a_recv.at[t], (fy, z)).wait_recv()
        to_core(t, fd, 0, half)
        remote(rows_of(fd, t, half, half), send_sem.at[t], b_recv.at[t], (fx, z)).wait_recv()
        to_core(t, fd, half, half)

    def multiply(t):
        whole = w_ref.at[t, pl.ds(0, 4 * line)]
        pltpu.make_async_copy(whole, whole, core_recv.at[t]).wait()
        blocks = normed_ref.shape[0] // 512
        column = pl.ds(pl.multiple_of((t % split) * LANES, LANES), LANES)

        def body(i, _):
            at = pl.ds(pl.multiple_of(i * 512, 512), 512)
            product = jnp.dot(normed_ref[at, :], w_ref[t], preferred_element_type=jnp.float32)

            @pl.when(t < split)
            def _():
                rec_ref[at, column] = product.astype(jnp.bfloat16)

            @pl.when(t >= split)
            def _():
                chunk = jnp.maximum(t - split, 0)
                state = b_ref[chunk, at, :] + a_ref[chunk, at, :] * start_ref[0:1, column]
                out_ref[at, column] = (state * jax.nn.gelu(product, approximate=True)).astype(out_ref.dtype)

            return 0

        lax.fori_loop(0, blocks, body, 0)

    def columns(h):
        return pl.ds(pl.multiple_of(h * channels, channels), channels)

    def tail_copy(h, source_rows, device):
        return pltpu.make_async_remote_copy(
            src_ref=rec_ref.at[pl.ds(source_rows, lead), columns(h)],
            dst_ref=before_ref.at[:, columns(h)],
            send_sem=tail_send.at[h], recv_sem=tail_recv.at[h],
            device_id=device, device_id_type=MESH,
        )

    def carry_copy(h, device):
        return pltpu.make_async_remote_copy(
            src_ref=carry_ref.at[:, columns(h)], dst_ref=start_ref.at[:, columns(h)],
            send_sem=carry_send.at[h], recv_sem=carry_recv.at[h],
            device_id=device, device_id_type=MESH,
        )

    def send_tail(h):
        @pl.when(z < nz - 1)
        def _():
            tail_copy(h, rows - lead, (f, z + 1)).start()

    def scan(h):
        @pl.when(z > 0)
        def _():
            tail_copy(h, rows - lead, (f, z)).wait_recv()

        cols = columns(h)
        padded_ref[pl.ds(0, lead), :] = before_ref[:, cols].astype(jnp.float32)
        padded_ref[pl.ds(lead, rows), :] = rec_ref[:, cols].astype(jnp.float32)
        conv_sum = jnp.zeros((rows, channels), jnp.float32) + bias_ref[:, cols]
        for tap in range(taps):
            conv_sum = conv_sum + weight_ref[tap : tap + 1, cols] * padded_ref[pl.ds(lead - tap, rows), :]
        conv_out = conv_sum.astype(jnp.bfloat16)
        gates = jnp.dot(conv_out, table_ref[cols, :], preferred_element_type=jnp.float32)
        input_gate = jax.nn.sigmoid(gates[:, :channels] + gate_bias_ref[0:1, cols])
        recur_gate = jax.nn.sigmoid(gates[:, channels:] + gate_bias_ref[1:2, cols])
        param = decay_ref[:, cols]
        softplus = jnp.maximum(param, 0.0) + jnp.log1p(jnp.exp(-jnp.abs(param)))
        log_decay = -8.0 * softplus * recur_gate
        decay = jnp.exp(log_decay)
        lost = -jnp.tanh(log_decay) * (decay * decay + 1.0)
        driven = jnp.sqrt(lost) * input_gate * conv_out.astype(jnp.float32)
        for j in range(pieces):
            a_ref[h * pieces + j] = decay[:, j * LANES : (j + 1) * LANES]
            b_ref[h * pieces + j] = driven[:, j * LANES : (j + 1) * LANES]

        lanes = 8
        length = rows // lanes

        def body(i, carry):
            at = pl.ds(i, lanes, stride=length)
            after = []
            for j in range(pieces):
                product, state = carry[j]
                decay_now = a_ref[h * pieces + j, at, :]
                product = product * decay_now
                state = decay_now * state + b_ref[h * pieces + j, at, :]
                a_ref[h * pieces + j, at, :] = product
                b_ref[h * pieces + j, at, :] = state
                after.append((product, state))
            return tuple(after)

        fresh = (jnp.ones((lanes, LANES), jnp.float32), jnp.zeros((lanes, LANES), jnp.float32))
        totals = lax.fori_loop(0, length, body, (fresh,) * pieces, unroll=8)
        for j in range(pieces):
            product, state = totals[j]
            start = jnp.zeros((1, LANES), jnp.float32)
            prefix = jnp.ones((1, LANES), jnp.float32)
            for i in range(lanes):
                at = pl.ds(i * length, length)
                within = a_ref[h * pieces + j, at, :]
                b_ref[h * pieces + j, at, :] = b_ref[h * pieces + j, at, :] + within * start
                a_ref[h * pieces + j, at, :] = within * prefix
                start = product[i : i + 1, :] * start + state[i : i + 1, :]
                prefix = prefix * product[i : i + 1, :]
            col = pl.ds(pl.multiple_of((h * pieces + j) * LANES, LANES), LANES)
            end_ref[0:1, col] = prefix
            end_ref[1:2, col] = start

    def make_carry(h):
        cols = columns(h)

        @pl.when(z > 0)
        def _():
            carry_copy(h, (f, z)).wait_recv()

        @pl.when(z < nz - 1)
        def _():
            end = end_ref[0:1, cols] * start_ref[0:1, cols] + end_ref[1:2, cols]
            carry_ref[:, cols] = jnp.broadcast_to(end, (carry_ref.shape[0], channels))

    def send_carry(h):
        @pl.when(z < nz - 1)
        def _():
            carry_copy(h, (f, z + 1)).start()

    @pl.when(z == 0)
    def _():
        before_ref[...] = jnp.zeros_like(before_ref)
        start_ref[...] = jnp.zeros_like(start_ref)

    stages = [z_first]
    for distance in range(1, nz):
        stages.append(functools.partial(z_hop, distance=distance))
    stages += [line_done, sides_done, corner_done, gate_done, multiply]
    lags = list(range(nz)) + [nz - 1, nz, nz + 1, nz + 1, nz + 2]
    scan_at = gate_steps + nz

    def on_head(s, first, stage):
        @pl.when((s >= first) & (s < first + pieces * heads) & ((s - first) % pieces == 0))
        def _():
            stage((s - first) // pieces)

    def step(s, _):
        for stage, lag in zip(stages[:-1], lags[:-1]):
            @pl.when((s >= lag) & (s < chunks + lag))
            def _():
                stage(s - lag)

        on_head(s, scan_at + 2 + 2 * z, send_carry)
        on_head(s, nz + 2 + pieces, send_tail)

        @pl.when(s < 4)
        def _():
            normalise(tokens_ref, gain_ref, normed_ref, s, 4)

        on_head(s, scan_at + 1 + 2 * z, make_carry)

        @pl.when((s >= lags[-1]) & (s < chunks + lags[-1]))
        def _():
            multiply(s - lags[-1])

        on_head(s, scan_at, scan)
        return 0

    lax.fori_loop(0, chunks + lags[-1], step, 0)

    def drain(t, _):
        for k in range(nz):
            shards_sent = (k + 1 if k < nz - 1 else 0) + (nz - k if k > 0 else 0)

            @pl.when(z == k)
            def _():
                sent = w_ref.at[t, pl.ds(0, shards_sent * shard + 3 * line)]
                pltpu.make_async_copy(sent, sent, send_sem.at[t]).wait()

                @pl.when(t < gate_steps)
                def _():
                    sent_gate = table_ref.at[pl.ds(0, shards_sent * piece)]
                    pltpu.make_async_copy(sent_gate, sent_gate, gate_send.at[t]).wait()

        whole = w_ref.at[t, pl.ds(0, 4 * line)]
        pltpu.make_async_copy(whole, whole, core_send.at[t]).wait()

        @pl.when(t < gate_steps)
        def _():
            others = table_ref.at[pl.ds(0, (nz - 1) * piece)]
            pltpu.make_async_copy(others, others, gate_core_send.at[t]).wait()

        @pl.when((t < heads) & (z < nz - 1))
        def _():
            tail_copy(t, rows - lead, (f, z)).wait_send()
            carry_copy(t, (f, z)).wait_send()

        return 0

    lax.fori_loop(0, chunks, drain, 0)


def fused_branch(
    nz, tokens, norm_gain, lru_proj, gelu_proj, conv_weight, conv_bias, gate_weights, gate_bias,
    decay_param,
):
    rows, width = tokens.shape
    inner = lru_proj.shape[1]
    chunks = 2 * inner // LANES
    channels = gate_weights.shape[1] // 2
    heads = inner // channels
    vmem = pl.BlockSpec(memory_space=pltpu.VMEM)
    any_ = pl.BlockSpec(memory_space=pl.ANY)
    dma = pltpu.SemaphoreType.DMA
    f32, bf16 = jnp.float32, jnp.bfloat16
    lead = 16
    return pl.pallas_call(
        functools.partial(branch_kernel, nz),
        out_shape=jax.ShapeDtypeStruct((rows, inner), bf16),
        in_specs=[vmem, vmem, any_, any_, any_, vmem, vmem, vmem, vmem],
        out_specs=vmem,
        scratch_shapes=[
            pltpu.VMEM((chunks, width, LANES), bf16),
            pltpu.VMEM((rows, width), bf16),
            pltpu.VMEM((rows, inner), bf16),
            pltpu.VMEM((gate_weights.shape[0] * nz, 2 * channels), bf16),
            pltpu.VMEM((lead, inner), bf16),
            pltpu.VMEM((lead + rows, channels), f32),
            pltpu.VMEM((chunks // 2, rows, LANES), f32),
            pltpu.VMEM((chunks // 2, rows, LANES), f32),
            pltpu.VMEM((8, inner), f32), pltpu.VMEM((8, inner), f32), pltpu.VMEM((8, inner), f32),
            dma((2,)), dma((chunks,)), dma((chunks,)), dma((chunks // 4,)), dma((chunks // 4,)),
            dma((heads,)), dma((heads,)),
            dma((chunks, nz)), dma((chunks // 4, nz)), dma((chunks // 4,)),
            dma((chunks,)), dma((chunks,)), dma((chunks,)), dma((chunks,)), dma((chunks,)),
            dma((heads,)), dma((heads,)),
        ],
        compiler_params=pltpu.CompilerParams(
            collective_id=0, has_side_effects=True, vmem_limit_bytes=VMEM_BYTES
        ),
    )(
        tokens, norm_gain.reshape(1, width), lru_proj, gelu_proj, gate_weights, conv_weight,
        conv_bias.reshape(1, inner), gate_bias, decay_param.reshape(1, inner),
    )


def scan_kernel(
    rec_ref, before_ref, weight_ref, bias_ref, table_ref, gate_bias_ref, decay_ref,
    state_ref, cumulative_ref, end_ref, padded_ref, a_ref, b_ref,
):
    rows, channels = rec_ref.shape
    taps = weight_ref.shape[0]
    lead = before_ref.shape[0]
    padded_ref[pl.ds(0, lead), :] = before_ref[...].astype(jnp.float32)
    padded_ref[pl.ds(lead, rows), :] = rec_ref[...].astype(jnp.float32)
    conv_sum = jnp.zeros((rows, channels), jnp.float32) + bias_ref[...]
    for tap in range(taps):
        conv_sum = conv_sum + weight_ref[tap : tap + 1, :] * padded_ref[pl.ds(lead - tap, rows), :]
    conv_out = conv_sum.astype(jnp.bfloat16)
    gates = jnp.dot(conv_out, table_ref[...], preferred_element_type=jnp.float32)
    input_gate = jax.nn.sigmoid(gates[:, :channels] + gate_bias_ref[0:1, :])
    recur_gate = jax.nn.sigmoid(gates[:, channels:] + gate_bias_ref[1:2, :])
    param = decay_ref[...]
    softplus = jnp.maximum(param, 0.0) + jnp.log1p(jnp.exp(-jnp.abs(param)))
    log_decay = -8.0 * softplus * recur_gate
    decay = jnp.exp(log_decay)
    lost = -jnp.tanh(log_decay) * (decay * decay + 1.0)
    driven = jnp.sqrt(lost) * input_gate * conv_out.astype(jnp.float32)
    parts = channels // LANES
    for j in range(parts):
        a_ref[j] = decay[:, j * LANES : (j + 1) * LANES]
        b_ref[j] = driven[:, j * LANES : (j + 1) * LANES]

    lanes = 8
    length = rows // lanes

    def body(i, carry):
        at = pl.ds(i, lanes, stride=length)
        after = []
        for j in range(parts):
            product, state = carry[j]
            decay_now = a_ref[j, at, :]
            product = product * decay_now
            state = decay_now * state + b_ref[j, at, :]
            a_ref[j, at, :] = product
            b_ref[j, at, :] = state
            after.append((product, state))
        return tuple(after)

    fresh = (jnp.ones((lanes, LANES), jnp.float32), jnp.zeros((lanes, LANES), jnp.float32))
    totals = lax.fori_loop(0, length, body, (fresh,) * parts, unroll=8)
    for j in range(parts):
        product, state = totals[j]
        cols = slice(j * LANES, (j + 1) * LANES)
        start = jnp.zeros((1, LANES), jnp.float32)
        prefix = jnp.ones((1, LANES), jnp.float32)
        for i in range(lanes):
            at = pl.ds(i * length, length)
            within = a_ref[j, at, :]
            state_ref[at, cols] = b_ref[j, at, :] + within * start
            cumulative_ref[at, cols] = within * prefix
            start = product[i : i + 1, :] * start + state[i : i + 1, :]
            prefix = prefix * product[i : i + 1, :]
        end_ref[0:1, cols] = prefix
        end_ref[1:2, cols] = start


def local_scan(rec, before, conv_weight, conv_bias, table, gate_bias, decay_param):
    rows, inner = rec.shape
    width = table.shape[1] // 2
    lead = before.shape[0]

    def columns(height):
        return pl.BlockSpec((height, width), lambda h: (0, h))

    return pl.pallas_call(
        scan_kernel,
        grid=(inner // width,),
        out_shape=(
            jax.ShapeDtypeStruct((rows, inner), jnp.float32),
            jax.ShapeDtypeStruct((rows, inner), jnp.float32),
            jax.ShapeDtypeStruct((2, inner), jnp.float32),
        ),
        in_specs=[
            columns(rows), columns(lead), columns(conv_weight.shape[0]), columns(1),
            pl.BlockSpec((width, 2 * width), lambda h: (h, 0)), columns(2), columns(1),
        ],
        out_specs=(columns(rows), columns(rows), columns(2)),
        scratch_shapes=[
            pltpu.VMEM((rows + lead, width), jnp.float32),
            pltpu.VMEM((width // LANES, rows, LANES), jnp.float32),
            pltpu.VMEM((width // LANES, rows, LANES), jnp.float32),
        ],
    )(
        rec, before, conv_weight, conv_bias.reshape(1, inner), table, gate_bias,
        decay_param.reshape(1, inner),
    )


def shards(
    nz, paired, tokens, norm_gain, lru_proj, gelu_proj, conv_weight, conv_bias, gate_weights,
    gate_bias, decay_param,
):
    seq_count, tok_rows, width = tokens.shape
    inner = lru_proj.shape[1]
    taps = conv_weight.shape[0]
    if paired:
        out = fused_branch(
            nz, tokens.reshape(tok_rows, width), norm_gain, lru_proj, gelu_proj, conv_weight,
            conv_bias, gate_weights, gate_bias, decay_param,
        )
        return out.reshape(seq_count, tok_rows, inner)
    flat = tokens.reshape(tok_rows, width).astype(jnp.float32)
    mean_square = jnp.mean(flat * flat, axis=-1, keepdims=True)
    normed = (flat * lax.rsqrt(mean_square + 1e-06) * norm_gain).astype(jnp.bfloat16)
    every = [
        lax.all_gather(w, ("fsdp", "seq"), axis=0, tiled=True) for w in (lru_proj, gelu_proj)
    ]
    rec = jnp.dot(normed, every[0], preferred_element_type=jnp.float32).astype(jnp.bfloat16)
    act = jnp.dot(normed, every[1], preferred_element_type=jnp.float32)
    table = lax.all_gather(gate_weights, "seq", axis=0, tiled=True)
    lead = 8
    before = lax.ppermute(
        rec[tok_rows - lead :, :], "seq", [(i, i + 1) for i in range(nz - 1)]
    )
    local, cumulative, ends = local_scan(
        rec, before, conv_weight, conv_bias, table, gate_bias, decay_param
    )
    every_end = lax.all_gather(ends, "seq")
    position = lax.axis_index("seq")
    start = jnp.zeros((inner,), jnp.float32)
    for k in range(nz - 1):
        start = jnp.where(k < position, every_end[k, 0] * start + every_end[k, 1], start)
    gelu = jax.nn.gelu(act, approximate=True)
    out = ((local + cumulative * start) * gelu).astype(jnp.bfloat16)
    return out.reshape(seq_count, tok_rows, inner)


def solution(mesh):
    placed = (
        P("fsdp", "seq", None), P(), P(("fsdp", "seq"), None), P(("fsdp", "seq"), None), P(), P(),
        P("seq", None), P(), P(),
    )
    nz = mesh.shape["seq"]
    paired = mesh.shape["fsdp"] == 8 and 1 < nz <= 5
    return jax.shard_map(
        functools.partial(shards, nz, paired), mesh=mesh, in_specs=placed,
        out_specs=P("fsdp", "seq", None), check_vma=False,
    )
```
